32 devices in a mesh: gx: 4 (over y, x), gy: 2 (over core), gz: 4 (over z).
Axes of the slice: x: 2, y: 2, z: 4, core: 2. Of those that a mesh axis runs over, the one named last changes fastest.
Arguments:
- populations: float32 [2, 19, 16, 32, 512], P(None, None, 'gx', 'gy', 'gz'), may hold values from 0.01 to 0.2
- solid: int32 [16, 32, 512], P('gx', 'gy', 'gz'), may hold values 0 or 1
Outputs:
- read: float32 [2, 19, 16, 32, 512], P(None, None, 'gx', 'gy', 'gz')
The draws below stay inside these ranges and needn't reach their ends.
All inputs are finite; a program needn't handle non-finite values. No bound on the sum of `solid` on one device may be relied on, other than what follows from the above.
Results may differ from the reference program's by a relative error of at most 0.0001.
Values sent between devices are 32-bit elements; how exact they have to be, the bound alone decides.
No kernel may reach another device: no remote copies, remote signals or barrier semaphores. Data moves between devices by JAX's collectives and lax.ppermute only.
A program may use at most 64 MiB of HBM per device.

```python
import math
import jax
import jax.numpy as jnp
import numpy as np
from jax import lax

NX = 16
NY = 32
NZ = 512


def touch_ends(values, own_key, smallest, high):
    extent = values.shape
    index_at = [jax.random.randint(jax.random.fold_in(own_key, axis), (), 0, extent[axis]) for axis in range(len(extent))]
    values = values.at[tuple(index_at)].set(smallest)
    longest = extent.index(max(extent))
    index_at[longest] = (index_at[longest] + 1) % extent[longest]
    return values.at[tuple(index_at)].set(high)


def steps_of(own_key, extent, shards, least, top_value):
    factor_of, own = 1.0, jax.random.fold_in(own_key, 6)
    for dim, blocks in shards:
        steps = jnp.exp(jax.random.uniform(jax.random.fold_in(own, dim), (blocks,), jnp.float32, least / len(shards), top_value / len(shards)))
        factor_of = factor_of * jnp.repeat(steps, extent[dim] // blocks).reshape([-1 if axis == dim else 1 for axis in range(len(extent))])
    return factor_of


def setup_inputs(seed: int = 0) -> dict:
    key_of = jax.random.split(jax.random.key(seed), 3)
    return {
        "populations": jnp.clip(jnp.exp(math.log(0.2) - 2.9957323 * jax.random.uniform(key_of[0], (2, 19, NX, NY, NZ), jnp.float32) ** steps_of(key_of[0], (2, 19, NX, NY, NZ), ((2, 4), (3, 2), (4, 4)), -0.2, 0.2)), 0.01, 0.2),
        "solid": touch_ends((jax.random.randint(key_of[1], (NX, NY, NZ), 0, 8) < 1).astype(jnp.int32), jax.random.fold_in(key_of[1], 1), 0, 1),
    }


VELOCITIES = [(0, 0, 0), (1, 0, 0), (-1, 0, 0), (0, 1, 0), (0, -1, 0), (0, 0, 1), (0, 0, -1),
              (1, 1, 0), (-1, -1, 0), (1, -1, 0), (-1, 1, 0), (1, 0, 1), (-1, 0, -1), (1, 0, -1),
              (-1, 0, 1), (0, 1, 1), (0, -1, -1), (0, 1, -1), (0, -1, 1)]
WEIGHTS = [1.0 / 3.0] + [1.0 / 18.0] * 6 + [1.0 / 36.0] * 12
OPPOSITE = [0, 2, 1, 4, 3, 6, 5, 8, 7, 10, 9, 12, 11, 14, 13, 16, 15, 18, 17]
coupling = 0.9
relax_times = (1.0, 0.8)
wall_values = (0.3, 1.5)


def collide(populations, fluid, psi, gradient):
    vel = jnp.asarray(np.array(VELOCITIES, np.float32))
    weights = jnp.asarray(np.array(WEIGHTS, np.float32))
    rho = jnp.sum(populations, axis=1)
    moment = jnp.einsum("ia,kixyz->kaxyz", vel, populations, precision=lax.Precision.HIGHEST)
    inv_first = 1.0 / relax_times[0]
    inv_second = 1.0 / relax_times[1]
    weight_sum = rho[0] * inv_first + rho[1] * inv_second
    common = (moment[0] * inv_first + moment[1] * inv_second) / weight_sum[None]
    forces = (-coupling * psi[0][None] * gradient[1], -coupling * psi[1][None] * gradient[0])
    results = []
    for comp in range(2):
        velocity = common + relax_times[comp] * forces[comp] / rho[comp][None]
        along = jnp.einsum("ia,axyz->ixyz", vel, velocity, precision=lax.Precision.HIGHEST)
        speed_sq = jnp.sum(velocity * velocity, axis=0)
        equil = weights[:, None, None, None] * rho[comp][None] * (
            1.0 + 3.0 * along + 4.5 * along * along - 1.5 * speed_sq[None])
        current = populations[comp]
        results.append(current - (current - equil) / relax_times[comp])
    post = jnp.stack(results, axis=0)
    return jnp.where(fluid[None, None], post, populations)


def reference(populations, solid):
    fluid = solid == 0
    rho = jnp.sum(populations, axis=1)
    wall = jnp.asarray(np.array(wall_values, np.float32)).reshape(2, 1, 1, 1)
    psi = jnp.where(fluid[None], rho, wall)
    parts = [jnp.zeros_like(psi) for axis_idx in range(3)]
    for i in range(1, 19):
        move = VELOCITIES[i]
        shifted = jnp.roll(psi, (-move[0], -move[1], -move[2]), axis=(1, 2, 3))
        for axis_idx in range(3):
            if move[axis_idx] != 0:
                parts[axis_idx] = parts[axis_idx] + (WEIGHTS[i] * move[axis_idx]) * shifted
    gradient = jnp.stack(parts, axis=1)
    post = collide(populations, fluid, psi, gradient)
    moved = []
    for i in range(19):
        move = VELOCITIES[i]
        pulled = jnp.roll(post[:, i], move, axis=(1, 2, 3))
        source_fluid = jnp.roll(fluid, move, axis=(0, 1, 2))
        moved.append(jnp.where(source_fluid[None], pulled, post[:, OPPOSITE[i]]))
    result = jnp.stack(moved, axis=1)
    return jnp.where(fluid[None, None], result, populations)
```

```python
import functools

import jax
import jax.numpy as jnp
from jax import lax
from jax.experimental import pallas as pl
from jax.experimental.pallas import tpu as pltpu
from jax.sharding import PartitionSpec as P

VEL = [
    (0, 0, 0),
    (1, 0, 0), (-1, 0, 0), (0, 1, 0), (0, -1, 0), (0, 0, 1), (0, 0, -1),
    (1, 1, 0), (-1, -1, 0), (1, -1, 0), (-1, 1, 0),
    (1, 0, 1), (-1, 0, -1), (1, 0, -1), (-1, 0, 1),
    (0, 1, 1), (0, -1, -1), (0, 1, -1), (0, -1, 1),
]
WEIGHT = [1.0 / 3.0] + [1.0 / 18.0] * 6 + [1.0 / 36.0] * 12
OPP = [0, 2, 1, 4, 3, 6, 5, 8, 7, 10, 9, 12, 11, 14, 13, 16, 15, 18, 17]
COUPLING = 0.9
TAU = (1.0, 0.8)
WALL = (0.3, 1.5)
W1, W2 = 1.0 / 18.0, 1.0 / 36.0
BLOCKED = 1e30
LIMIT = 1e29

XP = [i for i in range(19) if VEL[i][0] == 1]
XM = [i for i in range(19) if VEL[i][0] == -1]
ZP = [i for i in range(19) if VEL[i][2] == 1]
ZM = [i for i in range(19) if VEL[i][2] == -1]
YP = [i for i in range(19) if VEL[i][1] == 1]
YPAIR = [(i, VEL.index((VEL[i][0], -1, VEL[i][2]))) for i in YP]
HALO = 12


def lanes(shape):
    return lax.broadcasted_iota(jnp.int32, shape, len(shape) - 1)


def roll(v, shift, axis):
    shift = shift % v.shape[axis]
    return pltpu.roll(v, shift, axis) if shift else v


def up(v):
    return roll(v, -1, 0)


def down(v):
    return roll(v, 1, 0)


def fold(v, rows):
    tile = lax.broadcasted_iota(jnp.int32, (8, v.shape[1]), 0)
    return jnp.where(tile < 4, v[:8], v[rows - 8 : rows])


def parity(axis):
    return lax.rem(lax.axis_index(axis), 2) == 0


def put(sheet, value, source, target):
    return jnp.where(lanes(sheet.shape) == target, roll(value, target - source, 1), sheet)


def y_index(nx):
    wide, mid = nx + 4, nx + 2
    psi = lambda k, x: k * wide + x + 2
    com = lambda a, x: 2 * wide + a * mid + x + 1
    base = 2 * wide + 3 * mid
    pair = lambda j, x: base + j * nx + x
    low, high = base + 5 * nx, base + 5 * nx + 1
    return psi, com, pair, low, high, high + 1


def first_kernel(pop, solid, field, send_a, send_b, rows_out, sheets):
    nx, ny, nz = solid.shape
    wide = nx + 4
    psi, com, pair, _, _, _ = y_index(nx)
    for x in range(nx):
        fluid = solid[x] == 0
        q = []
        rho0 = rho1 = None
        for i in range(19):
            p0, p1 = pop[0, i, x], pop[1, i, x]
            rho0 = p0 if rho0 is None else rho0 + p0
            rho1 = p1 if rho1 is None else rho1 + p1
            q.append(p0 * (1.0 / TAU[0]) + p1 * (1.0 / TAU[1]))
        inverse = 1.0 / (rho0 * (1.0 / TAU[0]) + rho1 * (1.0 / TAU[1]))
        values = [jnp.where(fluid, rho0, -WALL[0]), jnp.where(fluid, rho1, -WALL[1])]
        for a in range(3):
            total = None
            for i in range(1, 19):
                if VEL[i][a] == 1:
                    term = q[i] - q[OPP[i]]
                    total = term if total is None else total + term
            values.append(total * inverse)
        for f in range(5):
            field[f, x] = values[f]
            rows_out[psi(f, x) if f < 2 else com(f - 2, x)] = fold(values[f], ny)
        for j, (plus, minus) in enumerate(YPAIR):
            tile = lax.broadcasted_iota(jnp.int32, (8, nz), 0)
            rows_out[pair(j, x)] = jnp.where(tile < 4, pop[1, minus, x, 0:8], pop[1, plus, x, ny - 8 : ny])
    even = parity("gx")
    high = [field[f, nx - 1] for f in range(5)] + [pop[1, i, nx - 1] for i in XP] + [field[f, nx - 2] for f in range(2)]
    low = [field[f, 0] for f in range(5)] + [pop[1, i, 0] for i in XM] + [field[f, 1] for f in range(2)]
    for f in range(HALO):
        send_a[f] = jnp.where(even, high[f], low[f])
        send_b[f] = jnp.where(even, low[f], high[f])
    for side, edge, inner, dirs in ((0, nz - 1, nz - 2, ZP), (1, 0, 1, ZM)):
        sheet = jnp.zeros((ny, nz), jnp.float32)
        for x in range(nx):
            for f in range(5):
                sheet = put(sheet, field[f, x], edge, f * wide + x + 2)
            for j, i in enumerate(dirs):
                sheet = put(sheet, pop[1, i, x], edge, (5 + j) * wide + x + 2)
            for k in range(2):
                sheet = put(sheet, field[k, x], inner, (10 + k) * wide + x + 2)
        sheets[side] = sheet


def sides(even, from_a, from_b, f):
    a, b = from_a[f], from_b[f]
    return jnp.where(even, a, b), jnp.where(even, b, a)


def y_kernel(nx, rows_in, from_a, from_b, rows_out):
    psi, com, pair, low, high, count = y_index(nx)
    ny = from_a.shape[1]
    even = parity("gx")
    for k in range(2):
        for x in range(nx):
            rows_out[psi(k, x)] = rows_in[psi(k, x)]
        above, below = sides(even, from_a, from_b, k)
        rows_out[psi(k, nx)], rows_out[psi(k, -1)] = fold(above, ny), fold(below, ny)
        above, below = sides(even, from_a, from_b, 10 + k)
        rows_out[psi(k, nx + 1)], rows_out[psi(k, -2)] = fold(above, ny), fold(below, ny)
    for a in range(3):
        for x in range(nx):
            rows_out[com(a, x)] = rows_in[com(a, x)]
        above, below = sides(even, from_a, from_b, 2 + a)
        rows_out[com(a, nx)], rows_out[com(a, -1)] = fold(above, ny), fold(below, ny)
    for j in range(5):
        for x in range(nx):
            rows_out[pair(j, x)] = rows_in[pair(j, x)]
    tile = lax.broadcasted_iota(jnp.int32, (8, from_a.shape[2]), 0)
    for where, step, dirs in ((low, 1, XP), (high, -1, XM)):
        plus, minus = dirs.index(VEL.index((step, 1, 0))) + 5, dirs.index(VEL.index((step, -1, 0))) + 5
        take = 1 if step == 1 else 0
        top, bottom = sides(even, from_a, from_b, minus)[take], sides(even, from_a, from_b, plus)[take]
        rows_out[where] = jnp.where(tile < 4, top[:8], bottom[ny - 8 :])


def merge_rows(y_even, from_y, n):
    if len(from_y) == 1:
        return from_y[0][n]
    a, b = from_y[0][n], from_y[1][n]
    tile = lax.broadcasted_iota(jnp.int32, a.shape, 0)
    return jnp.where((tile < 4) == y_even, a, b)


def z_kernel(nx, y_parts, sheets, from_a, from_b, *rest):
    from_y, (send_a, send_b) = rest[:y_parts], rest[y_parts:]
    psi, com, pair, low, high, _ = y_index(nx)
    wide = nx + 4
    nz = from_a.shape[2]
    x_even, y_even, z_even = parity("gx"), parity("gy"), parity("gz")
    rows = lambda n: merge_rows(y_even, from_y, n)
    above = lambda f: sides(x_even, from_a, from_b, f)[0]
    below = lambda f: sides(x_even, from_a, from_b, f)[1]
    made = []
    for side, edge, inner, dirs, cz in ((0, nz - 1, nz - 2, ZP, 1), (1, 0, 1, ZM, -1)):
        main = sheets[side]
        halo = jnp.zeros((8, nz), jnp.float32)
        for k in range(2):
            for f, lane in ((k, edge), (10 + k, inner)):
                main = put(main, below(k), lane, f * wide + 1)
                main = put(main, below(10 + k), lane, f * wide)
                main = put(main, above(k), lane, f * wide + nx + 2)
                main = put(main, above(10 + k), lane, f * wide + nx + 3)
                for x in range(-2, nx + 2):
                    halo = put(halo, rows(psi(k, x)), lane, f * wide + x + 2)
        for a in range(3):
            main = put(main, below(2 + a), edge, (2 + a) * wide + 1)
            main = put(main, above(2 + a), edge, (2 + a) * wide + nx + 2)
            for x in range(-1, nx + 1):
                halo = put(halo, rows(com(a, x)), edge, (2 + a) * wide + x + 2)
        for step, half, xs, source in ((1, XP, 1, below), (-1, XM, nx + 2, above)):
            i = VEL.index((step, 0, cz))
            main = put(main, source(5 + half.index(i)), edge, (5 + dirs.index(i)) * wide + xs)
        for j, (plus, minus) in enumerate(YPAIR):
            if VEL[plus][2] == cz:
                for x in range(nx):
                    tile = rows(pair(j, x))
                    halo = put(halo, tile, edge, (5 + dirs.index(plus)) * wide + x + 2)
                    halo = put(halo, tile, edge, (5 + dirs.index(minus)) * wide + x + 2)
        made.append(jnp.concatenate([main, halo], axis=0))
    send_a[...] = jnp.where(z_even, made[0], made[1])
    send_b[...] = jnp.where(z_even, made[1], made[0])


def posts(rho, vel, fluid, dirs, pop):
    out = {}
    for k in range(2):
        u = vel[k]
        base = rho[k] * (1.0 - 1.5 * (u[0] * u[0] + u[1] * u[1] + u[2] * u[2]))
        for i in dirs:
            rows = pop(k, i, True)
            cut = (lambda v: v[:rows]) if rows != rho[k].shape[0] else (lambda v: v)
            if i == 0:
                equil = base * WEIGHT[0]
            else:
                lead = next(a for a in range(3) if VEL[i][a])
                main = i if VEL[i][lead] == 1 else OPP[i]
                along = None
                for a in range(3):
                    c = VEL[main][a]
                    if c:
                        along = u[a] if along is None else (along + u[a] if c == 1 else along - u[a])
                flow = rho[k] * along
                even = base * WEIGHT[i] + (4.5 * WEIGHT[i]) * (flow * along)
                odd = (3.0 * WEIGHT[i]) * flow
                equil = even + odd if main == i else even - odd
            equil = cut(equil)
            if k == 0:
                post = equil
            else:
                post = (1.0 / TAU[1]) * equil + (1.0 - 1.0 / TAU[1]) * pop(k, i, False)
            out[k, i] = jnp.where(cut(fluid), post, BLOCKED)
    return out


def last_kernel(nx, y_parts, pop, solid, field, from_a, from_b, own_a, own_b, zf_a, zf_b, *rest):
    from_y, (out, t_ref, dy_ref, dz_ref, gy_ref, gz_ref, post_ref, edge_ref) = rest[:y_parts], rest[y_parts:]
    psi, com, pair, low, high, _ = y_index(nx)
    wide = nx + 4
    ny, nz = from_a.shape[1:]
    x_even, y_even, z_even = parity("gx"), parity("gy"), parity("gz")
    rows = lambda n: merge_rows(y_even, from_y, n)
    above = lambda f: sides(x_even, from_a, from_b, f)[0]
    below = lambda f: sides(x_even, from_a, from_b, f)[1]
    own_hi, own_lo = jnp.where(z_even, own_a[...], own_b[...]), jnp.where(z_even, own_b[...], own_a[...])
    z_hi, z_lo = jnp.where(z_even, zf_a[...], zf_b[...]), jnp.where(z_even, zf_b[...], zf_a[...])
    tall = (ny + 8, nz)

    def signed(k, x):
        if x < 0:
            main = below(k if x == -1 else 10 + k)
        elif x >= nx:
            main = above(k if x == nx else 10 + k)
        else:
            main = field[k, x]
        return jnp.concatenate([main, rows(psi(k, x))], axis=0)

    lane = lanes(tall)
    for k in range(2):
        for x in range(-2, nx + 2):
            a = jnp.abs(signed(k, x))
            column = k * wide + x + 2
            minus = jnp.where(lane == 0, jnp.abs(roll(z_lo, -column, 1)), roll(a, 1, 1))
            plus = jnp.where(lane == nz - 1, jnp.abs(roll(z_hi, nz - 1 - column, 1)), roll(a, -1, 1))
            a_up, a_down = up(a), down(a)
            z_sum, dz, dy = plus + minus, plus - minus, a_up - a_down
            t_ref[k, x + 2] = W1 * a + W2 * (a_up + a_down + z_sum)
            dy_ref[k, x + 2] = dy
            dz_ref[k, x + 2] = dz
            if -2 < x < nx + 1:
                gy_ref[k, x + 1] = W1 * dy + W2 * (up(z_sum) - down(z_sum))
                gz_ref[k, x + 1] = W1 * dz + W2 * (up(dz) + down(dz))

    for x in range(-1, nx + 1):
        gradient = []
        for k in range(2):
            gradient.append((
                t_ref[k, x + 3] - t_ref[k, x + 1],
                gy_ref[k, x + 1] + W2 * (dy_ref[k, x + 3] + dy_ref[k, x + 1]),
                gz_ref[k, x + 1] + W2 * (dz_ref[k, x + 3] + dz_ref[k, x + 1]),
            ))
        common = []
        for a in range(3):
            main = below(2 + a) if x < 0 else above(2 + a) if x == nx else field[2 + a, x]
            common.append(jnp.concatenate([main, rows(com(a, x))], axis=0))
        vel = [[common[a] - (COUPLING * TAU[k]) * gradient[1 - k][a] for a in range(3)] for k in range(2)]
        s0, s1 = signed(0, x), signed(1, x)

        def population(k, i, ask, x=x):
            if ask:
                return ny + 8 if VEL[i][1] else ny
            if x < 0:
                main = below(5 + XP.index(i))
            elif x == nx:
                main = above(5 + XM.index(i))
            else:
                main = pop[1, i, x]
            if not VEL[i][1]:
                return main
            j = next(j for j, both in enumerate(YPAIR) if i in both)
            return jnp.concatenate([main, rows(low if x < 0 else high if x == nx else pair(j, x))], axis=0)

        dirs = XP if x < 0 else XM if x == nx else range(19)
        for (k, i), value in posts((jnp.abs(s0), jnp.abs(s1)), vel, s0 > 0.0, dirs, population).items():
            post_ref[k, i, x + 1, 0 : value.shape[0]] = value

    for side, sheet, own, dirs in ((0, z_lo, own_lo, ZP), (1, z_hi, own_hi, ZM)):
        part = lambda s, f: roll(s, -f * wide, 1)
        gradient, sign = [], [part(sheet, 0), part(sheet, 1)]
        for k in range(2):
            a, beyond, inside = jnp.abs(sign[k]), jnp.abs(part(sheet, 10 + k)), jnp.abs(part(own, k))
            plus, minus = (inside, beyond) if side == 0 else (beyond, inside)
            a_up, a_down = up(a), down(a)
            z_sum, dz, dy = plus + minus, plus - minus, a_up - a_down
            t = W1 * a + W2 * (a_up + a_down + z_sum)
            right, left = (lambda v: roll(v, -1, 1)), (lambda v: roll(v, 1, 1))
            gradient.append((
                right(t) - left(t),
                W1 * dy + W2 * (up(z_sum) - down(z_sum) + right(dy) + left(dy)),
                W1 * dz + W2 * (up(dz) + down(dz) + right(dz) + left(dz)),
            ))
        common = [part(sheet, 2 + a) for a in range(3)]
        vel = [[common[a] - (COUPLING * TAU[k]) * gradient[1 - k][a] for a in range(3)] for k in range(2)]
        rho = (jnp.abs(sign[0]), jnp.abs(sign[1]))
        population = lambda k, i, ask: ny + 8 if ask else part(sheet, 5 + dirs.index(i))
        for (k, i), value in posts(rho, vel, sign[0] > 0.0, dirs, population).items():
            edge_ref[k, side, dirs.index(i)] = roll(value, VEL[i][1], 0)[:ny]

    lane = lanes((ny, nz))
    for x in range(nx):
        fluid = solid[x] == 0
        for k in range(2):
            for i in range(19):
                cx, cy, cz = VEL[i]
                source = x - cx
                if cy:
                    value = roll(post_ref[k, i, source + 1], cy, 0)[:ny]
                else:
                    value = post_ref[k, i, source + 1, 0:ny]
                if cz == 1:
                    edge = roll(edge_ref[k, 0, ZP.index(i)], -(source + 2), 1)
                    value = jnp.where(lane == 0, edge, roll(value, 1, 1))
                elif cz == -1:
                    edge = roll(edge_ref[k, 1, ZM.index(i)], nz - 1 - (source + 2), 1)
                    value = jnp.where(lane == nz - 1, edge, roll(value, -1, 1))
                if i:
                    value = jnp.where(value < LIMIT, value, post_ref[k, OPP[i], x + 1, 0:ny])
                out[k, i, x] = jnp.where(fluid, value, pop[k, i, x])


def swap(value, axis, count, first):
    pairs = [(i, (i + 1 if i % 2 == first else i - 1) % count) for i in range(count)]
    return lax.ppermute(value, axis, pairs)


def call(kernel, name, out_shape, *args, scratch=(), flops=200000):
    vmem = pl.BlockSpec(memory_space=pltpu.VMEM)
    return pl.pallas_call(
        kernel,
        name=name,
        out_shape=[jax.ShapeDtypeStruct(s, jnp.float32) for s in out_shape],
        in_specs=[vmem] * len(args),
        out_specs=[vmem] * len(out_shape),
        scratch_shapes=[pltpu.VMEM(s, jnp.float32) for s in scratch],
        compiler_params=pltpu.CompilerParams(vmem_limit_bytes=24 * 2**20),
        cost_estimate=pl.CostEstimate(flops=flops, bytes_accessed=flops, transcendentals=0),
    )(*args)


def body(sizes, pop, solid):
    nx, ny, nz = solid.shape
    count = y_index(nx)[-1]
    wide = nx + 4
    face = (HALO, ny, nz)
    field, send_a, send_b, rows, sheets = call(
        first_kernel, "local", [(5, nx, ny, nz), face, face, (count, 8, nz), (2, ny, nz)], pop, solid
    )
    from_a, from_b = swap(send_a, "gx", sizes["gx"], 0), swap(send_b, "gx", sizes["gx"], 1)
    (rows,) = call(functools.partial(y_kernel, nx), "rows", [(count, 8, nz)], rows, from_a, from_b)
    from_y = [swap(rows, "gy", sizes["gy"], 0)]
    if sizes["gy"] > 2:
        from_y.append(swap(rows, "gy", sizes["gy"], 1))
    y_parts = len(from_y)
    tall = (ny + 8, nz)
    own_a, own_b = call(
        functools.partial(z_kernel, nx, y_parts), "sheets", [tall, tall], sheets, from_a, from_b, *from_y
    )
    zf_b, zf_a = swap(own_b, "gz", sizes["gz"], 1), swap(own_a, "gz", sizes["gz"], 0)
    scratch = [(2, wide) + tall] * 3 + [(2, nx + 2) + tall] * 2 + [(2, 19, nx + 2) + tall, (2, 2, 5, ny, nz)]
    (result,) = call(
        functools.partial(last_kernel, nx, y_parts),
        "finish",
        [pop.shape],
        pop, solid, field, from_a, from_b, own_a, own_b, zf_a, zf_b, *from_y,
        scratch=scratch,
    )
    return result


def solution(mesh):
    sizes = dict(mesh.shape)
    assert all(n % 2 == 0 for n in sizes.values())
    spec = P(None, None, "gx", "gy", "gz")
    step = functools.partial(body, sizes)
    return jax.shard_map(step, mesh=mesh, in_specs=(spec, P("gx", "gy", "gz")), out_specs=spec, check_vma=False)
```

```python
import functools

import jax
import jax.numpy as jnp
from jax import lax
from jax.experimental import pallas as pl
from jax.experimental.pallas import tpu as pltpu
from jax.sharding import PartitionSpec as P


VEL = [
    (0, 0, 0),
    (1, 0, 0), (-1, 0, 0), (0, 1, 0), (0, -1, 0), (0, 0, 1), (0, 0, -1),
    (1, 1, 0), (-1, -1, 0), (1, -1, 0), (-1, 1, 0),
    (1, 0, 1), (-1, 0, -1), (1, 0, -1), (-1, 0, 1),
    (0, 1, 1), (0, -1, -1), (0, 1, -1), (0, -1, 1),
]
WEIGHT = [1.0 / 3.0] + [1.0 / 18.0] * 6 + [1.0 / 36.0] * 12
OPP = [0, 2, 1, 4, 3, 6, 5, 8, 7, 10, 9, 12, 11, 14, 13, 16, 15, 18, 17]
COUPLING = 0.9
TAU = (1.0, 0.8)
WALL = (0.3, 1.5)
W1, W2 = 1.0 / 18.0, 1.0 / 36.0
BLOCKED = 1e30
LIMIT = 1e29

XP = [i for i in range(19) if VEL[i][0] == 1]
XM = [i for i in range(19) if VEL[i][0] == -1]
ZP = [i for i in range(19) if VEL[i][2] == 1]
ZM = [i for i in range(19) if VEL[i][2] == -1]
YP = [i for i in range(19) if VEL[i][1] == 1]
YPAIR = [(i, VEL.index((VEL[i][0], -1, VEL[i][2]))) for i in YP]
HALO = 12


def lanes(shape):
    return lax.broadcasted_iota(jnp.int32, shape, len(shape) - 1)


def roll(v, shift, axis):
    shift = shift % v.shape[axis]
    return pltpu.roll(v, shift, axis) if shift else v


def up(v):
    return roll(v, -1, 0)


def down(v):
    return roll(v, 1, 0)


def fold(v, rows):
    tile = lax.broadcasted_iota(jnp.int32, (8, v.shape[1]), 0)
    return jnp.where(tile < 4, v[:8], v[rows - 8 : rows])


def parity(axis):
    return lax.rem(lax.axis_index(axis), 2) == 0


def put(sheet, value, source, target):
    return jnp.where(lanes(sheet.shape) == target, roll(value, target - source, 1), sheet)


def y_index(nx):
    wide, mid = nx + 4, nx + 2
    psi = lambda k, x: k * wide + x + 2
    com = lambda a, x: 2 * wide + a * mid + x + 1
    base = 2 * wide + 3 * mid
    pair = lambda j, x: base + j * nx + x
    low, high = base + 5 * nx, base + 5 * nx + 1
    return psi, com, pair, low, high, high + 1


def first_kernel(pop_hbm, solid_hbm, field, face_a, face_b, rim_a, rim_b, pop, solid, sems):
    nx, ny, nz = solid_hbm.shape
    wide = nx + 4
    flag_copy = pltpu.make_async_copy(solid_hbm, solid, sems.at[nx])
    copies = [pltpu.make_async_copy(pop_hbm.at[:, :, x], pop.at[:, :, x], sems.at[x]) for x in range(nx)]
    flag_copy.start()
    for x in range(nx):
        copies[x].start()
    flag_copy.wait()
    for x in range(nx):
        copies[x].wait()
        fluid = solid[x] == 0
        q = []
        rho0 = rho1 = None
        for i in range(19):
            p0, p1 = pop[0, i, x], pop[1, i, x]
            rho0 = p0 if rho0 is None else rho0 + p0
            rho1 = p1 if rho1 is None else rho1 + p1
            q.append(p0 * (1.0 / TAU[0]) + p1 * (1.0 / TAU[1]))
        inverse = 1.0 / (rho0 * (1.0 / TAU[0]) + rho1 * (1.0 / TAU[1]))
        field[0, x] = jnp.where(fluid, rho0, -WALL[0])
        field[1, x] = jnp.where(fluid, rho1, -WALL[1])
        for a in range(3):
            total = None
            for i in range(1, 19):
                if VEL[i][a] == 1:
                    term = q[i] - q[OPP[i]]
                    total = term if total is None else total + term
            field[2 + a, x] = total * inverse
    even = parity("gx")
    faces, rims = [], []
    for step, dirs, edge, inner in ((1, XP, nx - 1, nx - 2), (-1, XM, 0, 1)):
        face = [field[f, edge] for f in range(5)] + [pop[1, i, edge] for i in dirs] + [field[f, inner] for f in range(2)]
        rim = jnp.zeros((ny, nz), jnp.float32)
        for cz, z_dirs, z_edge, z_inner in ((1, ZP, nz - 1, nz - 2), (-1, ZM, 0, 1)):
            near, far = rim_lanes(wide, step, cz)
            for k in range(2):
                for f, lane in ((k, z_edge), (10 + k, z_inner)):
                    rim = put(rim, face[k], lane, f * wide + near)
                    rim = put(rim, face[10 + k], lane, f * wide + far)
            for a in range(3):
                rim = put(rim, face[2 + a], z_edge, (2 + a) * wide + near)
            i = VEL.index((step, 0, cz))
            rim = put(rim, face[5 + dirs.index(i)], z_edge, (5 + z_dirs.index(i)) * wide + near)
        faces.append(face)
        rims.append(rim)
    for f in range(HALO):
        face_a[f] = jnp.where(even, faces[0][f], faces[1][f])
        face_b[f] = jnp.where(even, faces[1][f], faces[0][f])
    rim_a[...] = jnp.where(even, rims[0], rims[1])
    rim_b[...] = jnp.where(even, rims[1], rims[0])


def rim_lanes(wide, step, cz):
    if step == 1:
        return (1, 0) if cz == 1 else (3, 2)
    return (wide - 2, wide - 1) if cz == 1 else (wide - 4, wide - 3)


def column_kernel(field, pop, sheets):
    nx, ny, nz = field.shape[1:]
    wide = nx + 4
    for side, edge, inner, dirs in ((0, nz - 1, nz - 2, ZP), (1, 0, 1, ZM)):
        sheet = jnp.zeros((ny, nz), jnp.float32)
        for x in range(nx):
            for f in range(5):
                sheet = put(sheet, field[f, x], edge, f * wide + x + 2)
            for j, i in enumerate(dirs):
                sheet = put(sheet, pop[1, i, x], edge, (5 + j) * wide + x + 2)
            for k in range(2):
                sheet = put(sheet, field[k, x], inner, (10 + k) * wide + x + 2)
        sheets[side] = sheet


def join_kernel(nx, sheets, from_a, from_b, joined, rows_out):
    ny = from_a.shape[0]
    wide = nx + 4
    even = parity("gx")
    a, b = from_a[...], from_b[...]
    above, below = jnp.where(even, a, b), jnp.where(even, b, a)
    place = lax.rem(lanes(a.shape), wide)
    for side, shift in ((0, 0), (1, 2)):
        sheet = jnp.where(place < 2, roll(below, -shift, 1), sheets[side])
        sheet = jnp.where(place >= nx + 2, roll(above, shift, 1), sheet)
        joined[side] = sheet
        rows_out[side] = fold(sheet, ny)


def sides(even, from_a, from_b, f):
    a, b = from_a[f], from_b[f]
    return jnp.where(even, a, b), jnp.where(even, b, a)


def y_kernel(nx, field, pop, from_a, from_b, rows_out):
    psi, com, pair, low, high, _ = y_index(nx)
    ny, nz = from_a.shape[1:]
    even = parity("gx")
    tile = lax.broadcasted_iota(jnp.int32, (8, nz), 0)
    for k in range(2):
        for x in range(nx):
            rows_out[psi(k, x)] = fold(field[k, x], ny)
        above, below = sides(even, from_a, from_b, k)
        rows_out[psi(k, nx)], rows_out[psi(k, -1)] = fold(above, ny), fold(below, ny)
        above, below = sides(even, from_a, from_b, 10 + k)
        rows_out[psi(k, nx + 1)], rows_out[psi(k, -2)] = fold(above, ny), fold(below, ny)
    for a in range(3):
        for x in range(nx):
            rows_out[com(a, x)] = fold(field[2 + a, x], ny)
        above, below = sides(even, from_a, from_b, 2 + a)
        rows_out[com(a, nx)], rows_out[com(a, -1)] = fold(above, ny), fold(below, ny)
    for j, (plus, minus) in enumerate(YPAIR):
        for x in range(nx):
            rows_out[pair(j, x)] = jnp.where(tile < 4, pop[1, minus, x, 0:8], pop[1, plus, x, ny - 8 : ny])
    for where, step, dirs in ((low, 1, XP), (high, -1, XM)):
        plus, minus = dirs.index(VEL.index((step, 1, 0))) + 5, dirs.index(VEL.index((step, -1, 0))) + 5
        take = 1 if step == 1 else 0
        top, bottom = sides(even, from_a, from_b, minus)[take], sides(even, from_a, from_b, plus)[take]
        rows_out[where] = jnp.where(tile < 4, top[:8], bottom[ny - 8 :])


def merge_rows(y_even, from_y, n):
    if len(from_y) == 1:
        return from_y[0][n]
    a, b = from_y[0][n], from_y[1][n]
    tile = lax.broadcasted_iota(jnp.int32, a.shape, 0)
    return jnp.where((tile < 4) == y_even, a, b)


def z_kernel(y_parts, joined, *rest):
    from_y, (send_a, send_b) = rest[:y_parts], rest[y_parts:]
    y_even, z_even = parity("gy"), parity("gz")
    made = [jnp.concatenate([joined[side], merge_rows(y_even, from_y, side)], axis=0) for side in range(2)]
    send_a[...] = jnp.where(z_even, made[0], made[1])
    send_b[...] = jnp.where(z_even, made[1], made[0])


def posts(rho, vel, fluid, dirs, pop):
    out = {}
    for k in range(2):
        u = vel[k]
        base = rho[k] * (1.0 - 1.5 * (u[0] * u[0] + u[1] * u[1] + u[2] * u[2]))
        for i in dirs:
            rows = pop(k, i, True)
            cut = (lambda v: v[:rows]) if rows != rho[k].shape[0] else (lambda v: v)
            if i == 0:
                equil = base * WEIGHT[0]
            else:
                lead = next(a for a in range(3) if VEL[i][a])
                main = i if VEL[i][lead] == 1 else OPP[i]
                along = None
                for a in range(3):
                    c = VEL[main][a]
                    if c:
                        along = u[a] if along is None else (along + u[a] if c == 1 else along - u[a])
                flow = rho[k] * along
                even = base * WEIGHT[i] + (4.5 * WEIGHT[i]) * (flow * along)
                odd = (3.0 * WEIGHT[i]) * flow
                equil = even + odd if main == i else even - odd
            equil = cut(equil)
            if k == 0:
                post = equil
            else:
                post = (1.0 / TAU[1]) * equil + (1.0 - 1.0 / TAU[1]) * pop(k, i, False)
            out[k, i] = jnp.where(cut(fluid), post, BLOCKED)
    return out


def last_kernel(nx, y_parts, pop, solid, field, from_a, from_b, own_a, own_b, zf_a, zf_b, *rest):
    from_y, (out_hbm, out, t_ref, dy_ref, dz_ref, gy_ref, gz_ref, post_ref, edge_ref, sems) = rest[:y_parts], rest[y_parts:]
    psi, com, pair, low, high, _ = y_index(nx)
    wide = nx + 4
    ny, nz = from_a.shape[1:]
    x_even, y_even, z_even = parity("gx"), parity("gy"), parity("gz")
    rows = lambda n: merge_rows(y_even, from_y, n)
    above = lambda f: sides(x_even, from_a, from_b, f)[0]
    below = lambda f: sides(x_even, from_a, from_b, f)[1]
    own_hi, own_lo = jnp.where(z_even, own_a[...], own_b[...]), jnp.where(z_even, own_b[...], own_a[...])
    z_hi, z_lo = jnp.where(z_even, zf_a[...], zf_b[...]), jnp.where(z_even, zf_b[...], zf_a[...])
    tall = (ny + 8, nz)

    def signed(k, x):
        if x < 0:
            main = below(k if x == -1 else 10 + k)
        elif x >= nx:
            main = above(k if x == nx else 10 + k)
        else:
            main = field[k, x]
        return jnp.concatenate([main, rows(psi(k, x))], axis=0)

    lane = lanes(tall)
    for k in range(2):
        for x in range(-2, nx + 2):
            a = jnp.abs(signed(k, x))
            column = k * wide + x + 2
            minus = jnp.where(lane == 0, jnp.abs(roll(z_lo, -column, 1)), roll(a, 1, 1))
            plus = jnp.where(lane == nz - 1, jnp.abs(roll(z_hi, nz - 1 - column, 1)), roll(a, -1, 1))
            a_up, a_down = up(a), down(a)
            z_sum, dz, dy = plus + minus, plus - minus, a_up - a_down
            t_ref[k, x + 2] = W1 * a + W2 * (a_up + a_down + z_sum)
            dy_ref[k, x + 2] = dy
            dz_ref[k, x + 2] = dz
            if -2 < x < nx + 1:
                gy_ref[k, x + 1] = W1 * dy + W2 * (up(z_sum) - down(z_sum))
                gz_ref[k, x + 1] = W1 * dz + W2 * (up(dz) + down(dz))

    for side, sheet, own, dirs in ((0, z_lo, own_lo, ZP), (1, z_hi, own_hi, ZM)):
        part = lambda s, f: roll(s, -f * wide, 1)
        gradient, sign = [], [part(sheet, 0), part(sheet, 1)]
        for k in range(2):
            a, beyond, inside = jnp.abs(sign[k]), jnp.abs(part(sheet, 10 + k)), jnp.abs(part(own, k))
            plus, minus = (inside, beyond) if side == 0 else (beyond, inside)
            a_up, a_down = up(a), down(a)
            z_sum, dz, dy = plus + minus, plus - minus, a_up - a_down
            t = W1 * a + W2 * (a_up + a_down + z_sum)
            right, left = (lambda v: roll(v, -1, 1)), (lambda v: roll(v, 1, 1))
            gradient.append((
                right(t) - left(t),
                W1 * dy + W2 * (up(z_sum) - down(z_sum) + right(dy) + left(dy)),
                W1 * dz + W2 * (up(dz) + down(dz) + right(dz) + left(dz)),
            ))
        common = [part(sheet, 2 + a) for a in range(3)]
        vel = [[common[a] - (COUPLING * TAU[k]) * gradient[1 - k][a] for a in range(3)] for k in range(2)]
        rho = (jnp.abs(sign[0]), jnp.abs(sign[1]))
        population = lambda k, i, ask: ny + 8 if ask else part(sheet, 5 + dirs.index(i))
        for (k, i), value in posts(rho, vel, sign[0] > 0.0, dirs, population).items():
            edge_ref[k, side, dirs.index(i)] = roll(value, VEL[i][1], 0)[:ny]

    lane_of = lanes((ny, nz))

    def finish(x):
        fluid = solid[x] == 0
        for k in range(2):
            for i in range(19):
                cx, cy, cz = VEL[i]
                source = x - cx
                if cy:
                    value = roll(post_ref[k, i, source + 1], cy, 0)[:ny]
                else:
                    value = post_ref[k, i, source + 1, 0:ny]
                if cz == 1:
                    edge = roll(edge_ref[k, 0, ZP.index(i)], -(source + 2), 1)
                    value = jnp.where(lane_of == 0, edge, roll(value, 1, 1))
                elif cz == -1:
                    edge = roll(edge_ref[k, 1, ZM.index(i)], nz - 1 - (source + 2), 1)
                    value = jnp.where(lane_of == nz - 1, edge, roll(value, -1, 1))
                if i:
                    value = jnp.where(value < LIMIT, value, post_ref[k, OPP[i], x + 1, 0:ny])
                out[k, i, x] = jnp.where(fluid, value, pop[k, i, x])
            pltpu.make_async_copy(out.at[k, :, x], out_hbm.at[k, :, x], sems.at[k, x]).start()

    for x in range(-1, nx + 1):
        gradient = []
        for k in range(2):
            gradient.append((
                t_ref[k, x + 3] - t_ref[k, x + 1],
                gy_ref[k, x + 1] + W2 * (dy_ref[k, x + 3] + dy_ref[k, x + 1]),
                gz_ref[k, x + 1] + W2 * (dz_ref[k, x + 3] + dz_ref[k, x + 1]),
            ))
        common = []
        for a in range(3):
            main = below(2 + a) if x < 0 else above(2 + a) if x == nx else field[2 + a, x]
            common.append(jnp.concatenate([main, rows(com(a, x))], axis=0))
        vel = [[common[a] - (COUPLING * TAU[k]) * gradient[1 - k][a] for a in range(3)] for k in range(2)]
        s0, s1 = signed(0, x), signed(1, x)

        def population(k, i, ask, x=x):
            if ask:
                return ny + 8 if VEL[i][1] else ny
            if x < 0:
                main = below(5 + XP.index(i))
            elif x == nx:
                main = above(5 + XM.index(i))
            else:
                main = pop[1, i, x]
            if not VEL[i][1]:
                return main
            j = next(j for j, both in enumerate(YPAIR) if i in both)
            return jnp.concatenate([main, rows(low if x < 0 else high if x == nx else pair(j, x))], axis=0)

        dirs = XP if x < 0 else XM if x == nx else range(19)
        for (k, i), value in posts((jnp.abs(s0), jnp.abs(s1)), vel, s0 > 0.0, dirs, population).items():
            post_ref[k, i, x + 1, 0 : value.shape[0]] = value
        if x > 0:
            finish(x - 1)
    for x in range(nx):
        for k in range(2):
            pltpu.make_async_copy(out.at[k, :, x], out_hbm.at[k, :, x], sems.at[k, x]).wait()


def swap(value, axis, count, first):
    pairs = [(i, (i + 1 if i % 2 == first else i - 1) % count) for i in range(count)]
    return lax.ppermute(value, axis, pairs)


def call(kernel, out_shape, *args, scratch=(), hbm_in=0, hbm_out=0, flops=200000, limit=16 * 2**20):
    space = lambda n, held: [pl.BlockSpec(memory_space=pltpu.HBM if j < held else pltpu.VMEM) for j in range(n)]
    args = [pltpu.with_memory_space_constraint(v, pltpu.HBM) if j < hbm_in else v for j, v in enumerate(args)]
    return pl.pallas_call(
        kernel,
        out_shape=[jax.ShapeDtypeStruct(*(s if isinstance(s[-1], type) else (s, jnp.float32))) for s in out_shape],
        in_specs=space(len(args), hbm_in),
        out_specs=space(len(out_shape), hbm_out),
        scratch_shapes=list(scratch),
        compiler_params=pltpu.CompilerParams(vmem_limit_bytes=limit),
        cost_estimate=pl.CostEstimate(flops=flops, bytes_accessed=flops, transcendentals=0),
    )(*args)


def body(sizes, pop, solid):
    return step(sizes, pop, solid)


def step(sizes, pop, solid):
    nx, ny, nz = solid.shape
    count = y_index(nx)[-1]
    wide = nx + 4
    face, plane, tall = (HALO, ny, nz), (ny, nz), (ny + 8, nz)
    gx, gy, gz = sizes["gx"], sizes["gy"], sizes["gz"]
    y_parts = 1 if gy == 2 else 2
    field, face_a, face_b, rim_a, rim_b, pop_v, solid_v = call(
        first_kernel,
        [(5, nx, ny, nz), face, face, plane, plane, pop.shape, (solid.shape, jnp.int32)],
        pop, solid,
        scratch=[pltpu.SemaphoreType.DMA((nx + 1,))],
        hbm_in=2,
    )
    rim_b, rim_a = swap(rim_b, "gx", gx, 1), swap(rim_a, "gx", gx, 0)
    face_b, face_a = swap(face_b, "gx", gx, 1), swap(face_a, "gx", gx, 0)
    (sheets,) = call(column_kernel, [(2,) + plane], field, pop_v)
    joined, ends = call(functools.partial(join_kernel, nx), [(2,) + plane, (2, 8, nz)], sheets, rim_a, rim_b)
    ends = [swap(ends, "gy", gy, m) for m in range(y_parts)]
    own_a, own_b = call(functools.partial(z_kernel, y_parts), [tall, tall], joined, *ends)
    far_b, far_a = swap(own_b, "gz", gz, 1), swap(own_a, "gz", gz, 0)
    (rows,) = call(functools.partial(y_kernel, nx), [(count, 8, nz)], field, pop_v, face_a, face_b)
    from_y = [swap(rows, "gy", gy, m) for m in range(y_parts)]
    vmem = lambda *s: pltpu.VMEM(s, jnp.float32)
    (result,) = call(
        functools.partial(last_kernel, nx, y_parts),
        [pop.shape],
        pop_v, solid_v, field, face_a, face_b, own_a, own_b, far_a, far_b, *from_y,
        scratch=[vmem(*pop.shape)]
        + [vmem(2, wide, *tall)] * 3
        + [vmem(2, nx + 2, *tall)] * 2
        + [vmem(2, 19, nx + 2, *tall), vmem(2, 2, 5, ny, nz), pltpu.SemaphoreType.DMA((2, nx))],
        hbm_out=1,
    )
    return result


def solution(mesh):
    sizes = dict(mesh.shape)
    assert all(n % 2 == 0 for n in sizes.values())
    spec = P(None, None, "gx", "gy", "gz")
    return jax.shard_map(
        functools.partial(body, sizes),
        mesh=mesh,
        in_specs=(spec, P("gx", "gy", "gz")),
        out_specs=spec,
        check_vma=False,
    )
```

```python
import functools

import jax
import jax.numpy as jnp
from jax import lax
from jax.experimental import pallas as pl
from jax.experimental.pallas import tpu as pltpu
from jax.sharding import PartitionSpec as P


VEL = [
    (0, 0, 0),
    (1, 0, 0), (-1, 0, 0), (0, 1, 0), (0, -1, 0), (0, 0, 1), (0, 0, -1),
    (1, 1, 0), (-1, -1, 0), (1, -1, 0), (-1, 1, 0),
    (1, 0, 1), (-1, 0, -1), (1, 0, -1), (-1, 0, 1),
    (0, 1, 1), (0, -1, -1), (0, 1, -1), (0, -1, 1),
]
WEIGHT = [1.0 / 3.0] + [1.0 / 18.0] * 6 + [1.0 / 36.0] * 12
OPP = [0, 2, 1, 4, 3, 6, 5, 8, 7, 10, 9, 12, 11, 14, 13, 16, 15, 18, 17]
COUPLING = 0.9
TAU = (1.0, 0.8)
WALL = (0.3, 1.5)
W1, W2 = 1.0 / 18.0, 1.0 / 36.0
BLOCKED = 1e30
LIMIT = 1e29

XP = [i for i in range(19) if VEL[i][0] == 1]
XM = [i for i in range(19) if VEL[i][0] == -1]
ZP = [i for i in range(19) if VEL[i][2] == 1]
ZM = [i for i in range(19) if VEL[i][2] == -1]
YP = [i for i in range(19) if VEL[i][1] == 1]
YPAIR = [(i, VEL.index((VEL[i][0], -1, VEL[i][2]))) for i in YP]
HALO = 12


def lanes(shape):
    return lax.broadcasted_iota(jnp.int32, shape, len(shape) - 1)


def roll(v, shift, axis):
    shift = shift % v.shape[axis]
    return pltpu.roll(v, shift, axis) if shift else v


def up(v):
    return roll(v, -1, 0)


def down(v):
    return roll(v, 1, 0)


def fold(v, rows):
    tile = lax.broadcasted_iota(jnp.int32, (8, v.shape[1]), 0)
    return jnp.where(tile < 4, v[:8], v[rows - 8 : rows])


def put(sheet, value, source, target):
    return jnp.where(lanes(sheet.shape) == target, roll(value, target - source, 1), sheet)


def y_index(nx):
    wide, mid = nx + 4, nx + 2
    psi = lambda k, x: k * wide + x + 2
    com = lambda a, x: 2 * wide + a * mid + x + 1
    base = 2 * wide + 3 * mid
    pair = lambda j, x: base + j * nx + x
    low, high = base + 5 * nx, base + 5 * nx + 1
    return psi, com, pair, low, high, high + 1


def first_kernel(pop_hbm, solid_hbm, field, face_high, face_low, rim_high, rim_low, pop, solid, sems):
    nx, ny, nz = solid_hbm.shape
    wide = nx + 4
    flag_copy = pltpu.make_async_copy(solid_hbm, solid, sems.at[nx])
    copies = [pltpu.make_async_copy(pop_hbm.at[:, :, x], pop.at[:, :, x], sems.at[x]) for x in range(nx)]
    flag_copy.start()
    for x in range(nx):
        copies[x].start()
    flag_copy.wait()
    for x in range(nx):
        copies[x].wait()
        fluid = solid[x] == 0
        q = []
        rho0 = rho1 = None
        for i in range(19):
            p0, p1 = pop[0, i, x], pop[1, i, x]
            rho0 = p0 if rho0 is None else rho0 + p0
            rho1 = p1 if rho1 is None else rho1 + p1
            q.append(p0 * (1.0 / TAU[0]) + p1 * (1.0 / TAU[1]))
        inverse = 1.0 / (rho0 * (1.0 / TAU[0]) + rho1 * (1.0 / TAU[1]))
        field[0, x] = jnp.where(fluid, rho0, -WALL[0])
        field[1, x] = jnp.where(fluid, rho1, -WALL[1])
        for a in range(3):
            total = None
            for i in range(1, 19):
                if VEL[i][a] == 1:
                    term = q[i] - q[OPP[i]]
                    total = term if total is None else total + term
            field[2 + a, x] = total * inverse
    for step, dirs, edge, inner, face_out, rim_out in (
        (1, XP, nx - 1, nx - 2, face_high, rim_high),
        (-1, XM, 0, 1, face_low, rim_low),
    ):
        face = [field[f, edge] for f in range(5)] + [pop[1, i, edge] for i in dirs] + [field[f, inner] for f in range(2)]
        rim = jnp.zeros((ny, nz), jnp.float32)
        for cz, z_dirs, z_edge, z_inner in ((1, ZP, nz - 1, nz - 2), (-1, ZM, 0, 1)):
            near, far = rim_lanes(wide, step, cz)
            for k in range(2):
                for f, lane in ((k, z_edge), (10 + k, z_inner)):
                    rim = put(rim, face[k], lane, f * wide + near)
                    rim = put(rim, face[10 + k], lane, f * wide + far)
            for a in range(3):
                rim = put(rim, face[2 + a], z_edge, (2 + a) * wide + near)
            i = VEL.index((step, 0, cz))
            rim = put(rim, face[5 + dirs.index(i)], z_edge, (5 + z_dirs.index(i)) * wide + near)
        for f in range(HALO):
            face_out[f] = face[f]
        rim_out[...] = rim


def rim_lanes(wide, step, cz):
    if step == 1:
        return (1, 0) if cz == 1 else (3, 2)
    return (wide - 2, wide - 1) if cz == 1 else (wide - 4, wide - 3)


def column_kernel(field, pop, sheets):
    nx, ny, nz = field.shape[1:]
    wide = nx + 4
    for side, edge, inner, dirs in ((0, nz - 1, nz - 2, ZP), (1, 0, 1, ZM)):
        sheet = jnp.zeros((ny, nz), jnp.float32)
        for x in range(nx):
            for f in range(5):
                sheet = put(sheet, field[f, x], edge, f * wide + x + 2)
            for j, i in enumerate(dirs):
                sheet = put(sheet, pop[1, i, x], edge, (5 + j) * wide + x + 2)
            for k in range(2):
                sheet = put(sheet, field[k, x], inner, (10 + k) * wide + x + 2)
        sheets[side] = sheet


def join_kernel(nx, sheets, from_below, from_above, joined, rows_out):
    below, above = from_below[...], from_above[...]
    ny = below.shape[0]
    wide = nx + 4
    place = lax.rem(lanes(below.shape), wide)
    for side, shift in ((0, 0), (1, 2)):
        sheet = jnp.where(place < 2, roll(below, -shift, 1), sheets[side])
        sheet = jnp.where(place >= nx + 2, roll(above, shift, 1), sheet)
        joined[side] = sheet
        rows_out[side] = fold(sheet, ny)


def y_kernel(nx, field, pop, from_below, from_above, rows_out):
    psi, com, pair, low, high, _ = y_index(nx)
    below, above = (lambda f: from_below[f]), (lambda f: from_above[f])
    ny, nz = field.shape[2:]
    tile = lax.broadcasted_iota(jnp.int32, (8, nz), 0)
    for k in range(2):
        for x in range(nx):
            rows_out[psi(k, x)] = fold(field[k, x], ny)
        rows_out[psi(k, nx)], rows_out[psi(k, -1)] = fold(above(k), ny), fold(below(k), ny)
        rows_out[psi(k, nx + 1)], rows_out[psi(k, -2)] = fold(above(10 + k), ny), fold(below(10 + k), ny)
    for a in range(3):
        for x in range(nx):
            rows_out[com(a, x)] = fold(field[2 + a, x], ny)
        rows_out[com(a, nx)], rows_out[com(a, -1)] = fold(above(2 + a), ny), fold(below(2 + a), ny)
    for j, (plus, minus) in enumerate(YPAIR):
        for x in range(nx):
            rows_out[pair(j, x)] = jnp.where(tile < 4, pop[1, minus, x, 0:8], pop[1, plus, x, ny - 8 : ny])
    for where, source, step, dirs in ((low, below, 1, XP), (high, above, -1, XM)):
        plus, minus = dirs.index(VEL.index((step, 1, 0))) + 5, dirs.index(VEL.index((step, -1, 0))) + 5
        rows_out[where] = jnp.where(tile < 4, source(minus)[:8], source(plus)[ny - 8 :])


def merge_rows(from_y, n):
    if len(from_y) == 1:
        return from_y[0][n]
    below, above = from_y[0][n], from_y[1][n]
    return jnp.where(lax.broadcasted_iota(jnp.int32, above.shape, 0) < 4, above, below)


def z_kernel(y_parts, joined, *rest):
    from_y, (send_high, send_low) = rest[:y_parts], rest[y_parts:]
    for side, send in ((0, send_high), (1, send_low)):
        send[...] = jnp.concatenate([joined[side], merge_rows(from_y, side)], axis=0)


def posts(rho, vel, fluid, dirs, pop):
    out = {}
    for k in range(2):
        u = vel[k]
        base = rho[k] * (1.0 - 1.5 * (u[0] * u[0] + u[1] * u[1] + u[2] * u[2]))
        for i in dirs:
            rows = pop(k, i, True)
            cut = (lambda v: v[:rows]) if rows != rho[k].shape[0] else (lambda v: v)
            if i == 0:
                equil = base * WEIGHT[0]
            else:
                lead = next(a for a in range(3) if VEL[i][a])
                main = i if VEL[i][lead] == 1 else OPP[i]
                along = None
                for a in range(3):
                    c = VEL[main][a]
                    if c:
                        along = u[a] if along is None else (along + u[a] if c == 1 else along - u[a])
                flow = rho[k] * along
                even = base * WEIGHT[i] + (4.5 * WEIGHT[i]) * (flow * along)
                odd = (3.0 * WEIGHT[i]) * flow
                equil = even + odd if main == i else even - odd
            equil = cut(equil)
            if k == 0:
                post = equil
            else:
                post = (1.0 / TAU[1]) * equil + (1.0 - 1.0 / TAU[1]) * pop(k, i, False)
            out[k, i] = jnp.where(cut(fluid), post, BLOCKED)
    return out


def last_kernel(nx, y_parts, pop, solid, field, own_high, own_low, from_below, from_above, z_low, z_high, *rest):
    below, above = (lambda f: from_below[f]), (lambda f: from_above[f])
    from_y, (out_hbm, out, t_ref, dy_ref, dz_ref, gy_ref, gz_ref, post_ref, edge_ref, sems) = rest[:y_parts], rest[y_parts:]
    psi, com, pair, low, high, _ = y_index(nx)
    wide = nx + 4
    ny, nz = field.shape[2:]
    rows = lambda n: merge_rows(from_y, n)
    own_hi, own_lo, z_lo, z_hi = own_high[...], own_low[...], z_low[...], z_high[...]
    tall = (ny + 8, nz)

    def signed(k, x):
        if x < 0:
            main = below(k if x == -1 else 10 + k)
        elif x >= nx:
            main = above(k if x == nx else 10 + k)
        else:
            main = field[k, x]
        return jnp.concatenate([main, rows(psi(k, x))], axis=0)

    lane = lanes(tall)
    for k in range(2):
        for x in range(-2, nx + 2):
            a = jnp.abs(signed(k, x))
            column = k * wide + x + 2
            minus = jnp.where(lane == 0, jnp.abs(roll(z_lo, -column, 1)), roll(a, 1, 1))
            plus = jnp.where(lane == nz - 1, jnp.abs(roll(z_hi, nz - 1 - column, 1)), roll(a, -1, 1))
            a_up, a_down = up(a), down(a)
            z_sum, dz, dy = plus + minus, plus - minus, a_up - a_down
            t_ref[k, x + 2] = W1 * a + W2 * (a_up + a_down + z_sum)
            dy_ref[k, x + 2] = dy
            dz_ref[k, x + 2] = dz
            if -2 < x < nx + 1:
                gy_ref[k, x + 1] = W1 * dy + W2 * (up(z_sum) - down(z_sum))
                gz_ref[k, x + 1] = W1 * dz + W2 * (up(dz) + down(dz))

    for side, sheet, own, dirs in ((0, z_lo, own_lo, ZP), (1, z_hi, own_hi, ZM)):
        part = lambda s, f: roll(s, -f * wide, 1)
        gradient, sign = [], [part(sheet, 0), part(sheet, 1)]
        for k in range(2):
            a, beyond, inside = jnp.abs(sign[k]), jnp.abs(part(sheet, 10 + k)), jnp.abs(part(own, k))
            plus, minus = (inside, beyond) if side == 0 else (beyond, inside)
            a_up, a_down = up(a), down(a)
            z_sum, dz, dy = plus + minus, plus - minus, a_up - a_down
            t = W1 * a + W2 * (a_up + a_down + z_sum)
            right, left = (lambda v: roll(v, -1, 1)), (lambda v: roll(v, 1, 1))
            gradient.append((
                right(t) - left(t),
                W1 * dy + W2 * (up(z_sum) - down(z_sum) + right(dy) + left(dy)),
                W1 * dz + W2 * (up(dz) + down(dz) + right(dz) + left(dz)),
            ))
        common = [part(sheet, 2 + a) for a in range(3)]
        vel = [[common[a] - (COUPLING * TAU[k]) * gradient[1 - k][a] for a in range(3)] for k in range(2)]
        rho = (jnp.abs(sign[0]), jnp.abs(sign[1]))
        population = lambda k, i, ask: ny + 8 if ask else part(sheet, 5 + dirs.index(i))
        for (k, i), value in posts(rho, vel, sign[0] > 0.0, dirs, population).items():
            edge_ref[k, side, dirs.index(i)] = roll(value, VEL[i][1], 0)[:ny]

    lane_of = lanes((ny, nz))

    def finish(x):
        fluid = solid[x] == 0
        for k in range(2):
            for i in range(19):
                cx, cy, cz = VEL[i]
                source = x - cx
                if cy:
                    value = roll(post_ref[k, i, source + 1], cy, 0)[:ny]
                else:
                    value = post_ref[k, i, source + 1, 0:ny]
                if cz == 1:
                    edge = roll(edge_ref[k, 0, ZP.index(i)], -(source + 2), 1)
                    value = jnp.where(lane_of == 0, edge, roll(value, 1, 1))
                elif cz == -1:
                    edge = roll(edge_ref[k, 1, ZM.index(i)], nz - 1 - (source + 2), 1)
                    value = jnp.where(lane_of == nz - 1, edge, roll(value, -1, 1))
                if i:
                    value = jnp.where(value < LIMIT, value, post_ref[k, OPP[i], x + 1, 0:ny])
                out[k, i, x] = jnp.where(fluid, value, pop[k, i, x])
            pltpu.make_async_copy(out.at[k, :, x], out_hbm.at[k, :, x], sems.at[k, x]).start()

    for x in range(-1, nx + 1):
        gradient = []
        for k in range(2):
            gradient.append((
                t_ref[k, x + 3] - t_ref[k, x + 1],
                gy_ref[k, x + 1] + W2 * (dy_ref[k, x + 3] + dy_ref[k, x + 1]),
                gz_ref[k, x + 1] + W2 * (dz_ref[k, x + 3] + dz_ref[k, x + 1]),
            ))
        common = []
        for a in range(3):
            main = below(2 + a) if x < 0 else above(2 + a) if x == nx else field[2 + a, x]
            common.append(jnp.concatenate([main, rows(com(a, x))], axis=0))
        vel = [[common[a] - (COUPLING * TAU[k]) * gradient[1 - k][a] for a in range(3)] for k in range(2)]
        s0, s1 = signed(0, x), signed(1, x)

        def population(k, i, ask, x=x):
            if ask:
                return ny + 8 if VEL[i][1] else ny
            if x < 0:
                main = below(5 + XP.index(i))
            elif x == nx:
                main = above(5 + XM.index(i))
            else:
                main = pop[1, i, x]
            if not VEL[i][1]:
                return main
            j = next(j for j, both in enumerate(YPAIR) if i in both)
            return jnp.concatenate([main, rows(low if x < 0 else high if x == nx else pair(j, x))], axis=0)

        dirs = XP if x < 0 else XM if x == nx else range(19)
        for (k, i), value in posts((jnp.abs(s0), jnp.abs(s1)), vel, s0 > 0.0, dirs, population).items():
            post_ref[k, i, x + 1, 0 : value.shape[0]] = value
        if x > 0:
            finish(x - 1)
    for x in range(nx):
        for k in range(2):
            pltpu.make_async_copy(out.at[k, :, x], out_hbm.at[k, :, x], sems.at[k, x]).wait()


def ring(value, axis, count, step):
    return lax.ppermute(value, axis, [(i, (i + step) % count) for i in range(count)])


def spread(high, low, axis, count):
    return ring(high, axis, count, 1), ring(low, axis, count, -1)


def spread_rows(rows, count):
    return spread(rows, rows, "gy", count) if count > 2 else (ring(rows, "gy", count, 1),)


def call(kernel, out_shape, *args, scratch=(), hbm_in=0, hbm_out=0, flops=200000, limit=16 * 2**20):
    space = lambda n, held: [pl.BlockSpec(memory_space=pltpu.HBM if j < held else pltpu.VMEM) for j in range(n)]
    args = [pltpu.with_memory_space_constraint(v, pltpu.HBM) if j < hbm_in else v for j, v in enumerate(args)]
    return pl.pallas_call(
        kernel,
        out_shape=[jax.ShapeDtypeStruct(*(s if isinstance(s[-1], type) else (s, jnp.float32))) for s in out_shape],
        in_specs=space(len(args), hbm_in),
        out_specs=space(len(out_shape), hbm_out),
        scratch_shapes=list(scratch),
        compiler_params=pltpu.CompilerParams(vmem_limit_bytes=limit),
        cost_estimate=pl.CostEstimate(flops=flops, bytes_accessed=flops, transcendentals=0),
    )(*args)


def body(sizes, pop, solid):
    return step(sizes, pop, solid)


def step(sizes, pop, solid):
    nx, ny, nz = solid.shape
    count = y_index(nx)[-1]
    wide = nx + 4
    face, plane, tall = (HALO, ny, nz), (ny, nz), (ny + 8, nz)
    gx, gy, gz = sizes["gx"], sizes["gy"], sizes["gz"]
    y_parts = 1 if gy == 2 else 2
    field, face_high, face_low, rim_high, rim_low, pop_v, solid_v = call(
        first_kernel,
        [(5, nx, ny, nz), face, face, plane, plane, pop.shape, (solid.shape, jnp.int32)],
        pop, solid,
        scratch=[pltpu.SemaphoreType.DMA((nx + 1,))],
        hbm_in=2,
    )
    rims = spread(rim_high, rim_low, "gx", gx)
    faces = spread(face_high, face_low, "gx", gx)
    (sheets,) = call(column_kernel, [(2,) + plane], field, pop_v)
    joined, ends = call(functools.partial(join_kernel, nx), [(2,) + plane, (2, 8, nz)], sheets, *rims)
    ends = spread_rows(ends, gy)
    own = call(functools.partial(z_kernel, y_parts), [tall, tall], joined, *ends)
    far = spread(*own, "gz", gz)
    (rows,) = call(functools.partial(y_kernel, nx), [(count, 8, nz)], field, pop_v, *faces)
    from_y = spread_rows(rows, gy)
    vmem = lambda *s: pltpu.VMEM(s, jnp.float32)
    (result,) = call(
        functools.partial(last_kernel, nx, y_parts),
        [pop.shape],
        pop_v, solid_v, field, *own, *faces, *far, *from_y,
        scratch=[vmem(*pop.shape)]
        + [vmem(2, wide, *tall)] * 3
        + [vmem(2, nx + 2, *tall)] * 2
        + [vmem(2, 19, nx + 2, *tall), vmem(2, 2, 5, ny, nz), pltpu.SemaphoreType.DMA((2, nx))],
        hbm_out=1,
    )
    return result


def solution(mesh):
    sizes = dict(mesh.shape)
    spec = P(None, None, "gx", "gy", "gz")
    return jax.shard_map(
        functools.partial(body, sizes),
        mesh=mesh,
        in_specs=(spec, P("gx", "gy", "gz")),
        out_specs=spec,
        check_vma=False,
    )
```

```python
import functools

import jax
import jax.numpy as jnp
from jax import lax
from jax.experimental import pallas as pl
from jax.experimental.pallas import tpu as pltpu
from jax.sharding import PartitionSpec as P


VEL = [
    (0, 0, 0),
    (1, 0, 0), (-1, 0, 0), (0, 1, 0), (0, -1, 0), (0, 0, 1), (0, 0, -1),
    (1, 1, 0), (-1, -1, 0), (1, -1, 0), (-1, 1, 0),
    (1, 0, 1), (-1, 0, -1), (1, 0, -1), (-1, 0, 1),
    (0, 1, 1), (0, -1, -1), (0, 1, -1), (0, -1, 1),
]
WEIGHT = [1.0 / 3.0] + [1.0 / 18.0] * 6 + [1.0 / 36.0] * 12
OPP = [0, 2, 1, 4, 3, 6, 5, 8, 7, 10, 9, 12, 11, 14, 13, 16, 15, 18, 17]
COUPLING = 0.9
TAU = (1.0, 0.8)
WALL = (0.3, 1.5)
W1, W2 = 1.0 / 18.0, 1.0 / 36.0
BLOCKED = 1e32
LIMIT = 1e29

XP = [i for i in range(19) if VEL[i][0] == 1]
XM = [i for i in range(19) if VEL[i][0] == -1]
ZP = [i for i in range(19) if VEL[i][2] == 1]
ZM = [i for i in range(19) if VEL[i][2] == -1]
YP = [i for i in range(19) if VEL[i][1] == 1]
YPAIR = [(i, VEL.index((VEL[i][0], -1, VEL[i][2]))) for i in YP]


def mirror(i):
    return VEL.index((VEL[i][0], VEL[i][1], -VEL[i][2]))


HALO = 12


def lanes(shape):
    return lax.broadcasted_iota(jnp.int32, shape, len(shape) - 1)


def roll(v, shift, axis):
    shift = shift % v.shape[axis]
    return pltpu.roll(v, shift, axis) if shift else v


def up(v):
    return roll(v, -1, 0)


def down(v):
    return roll(v, 1, 0)


def fold(v, rows):
    tile = lax.broadcasted_iota(jnp.int32, (8, v.shape[1]), 0)
    return jnp.where(tile < 4, v[:8], v[rows - 8 : rows])


def put(sheet, value, source, target):
    return jnp.where(lanes(sheet.shape) == target, roll(value, target - source, 1), sheet)


def y_index(nx):
    wide, mid = nx + 4, nx + 2
    psi = lambda k, x: k * wide + x + 2
    com = lambda a, x: 2 * wide + a * mid + x + 1
    base = 2 * wide + 3 * mid
    pair = lambda j, x: base + j * nx + x
    low, high = base + 5 * nx, base + 5 * nx + 1
    return psi, com, pair, low, high, high + 1


def first_kernel(pop_hbm, solid_hbm, field, face_high, face_low, rim_high, rim_low, pop, solid, sems):
    nx, ny, nz = solid_hbm.shape
    wide = nx + 4

    def face_side(step, dirs, edge, inner, face_out, rim_out):
        face = [field[f, edge] for f in range(5)] + [pop[1, i, edge] for i in dirs] + [field[f, inner] for f in range(2)]
        rim = jnp.zeros((ny, nz), jnp.float32)
        for cz, z_dirs, z_edge, z_inner in ((1, ZP, nz - 1, nz - 2), (-1, ZM, 0, 1)):
            near, far = rim_lanes(wide, step, cz)
            for k in range(2):
                for f, lane in ((k, z_edge), (10 + k, z_inner)):
                    rim = put(rim, face[k], lane, f * wide + near)
                    rim = put(rim, face[10 + k], lane, f * wide + far)
            for a in range(3):
                rim = put(rim, face[2 + a], z_edge, (2 + a) * wide + near)
            i = VEL.index((step, 0, cz))
            rim = put(rim, face[5 + dirs.index(i)], z_edge, (5 + z_dirs.index(i)) * wide + near)
        for f in range(HALO):
            face_out[f] = face[f]
        rim_out[...] = rim

    flag_copy = pltpu.make_async_copy(solid_hbm, solid, sems.at[nx])
    copies = [pltpu.make_async_copy(pop_hbm.at[:, :, x], pop.at[:, :, x], sems.at[x]) for x in range(nx)]
    flag_copy.start()
    for x in range(nx):
        copies[x].start()
    flag_copy.wait()
    for x in range(nx):
        copies[x].wait()
        fluid = solid[x] == 0
        q = []
        rho0 = rho1 = None
        for i in range(19):
            p0, p1 = pop[0, i, x], pop[1, i, x]
            rho0 = p0 if rho0 is None else rho0 + p0
            rho1 = p1 if rho1 is None else rho1 + p1
            q.append(p0 * (1.0 / TAU[0]) + p1 * (1.0 / TAU[1]))
        inverse = 1.0 / (rho0 * (1.0 / TAU[0]) + rho1 * (1.0 / TAU[1]))
        field[0, x] = jnp.where(fluid, rho0, -WALL[0])
        field[1, x] = jnp.where(fluid, rho1, -WALL[1])
        for a in range(3):
            total = None
            for i in range(1, 19):
                if VEL[i][a] == 1:
                    term = q[i] - q[OPP[i]]
                    total = term if total is None else total + term
            field[2 + a, x] = total * inverse
        if x == 1:
            face_side(-1, XM, 0, 1, face_low, rim_low)
    face_side(1, XP, nx - 1, nx - 2, face_high, rim_high)


def rim_lanes(wide, step, cz):
    if step == 1:
        return (1, 0) if cz == 1 else (3, 2)
    return (wide - 2, wide - 1) if cz == 1 else (wide - 4, wide - 3)


def column_kernel(field, pop, sheets):
    nx, ny, nz = field.shape[1:]
    wide = nx + 4
    for side, edge, inner, dirs in ((0, nz - 1, nz - 2, ZP), (1, 0, 1, ZM)):
        sheet = jnp.zeros((ny, nz), jnp.float32)
        for x in range(nx):
            for f in range(5):
                sheet = put(sheet, field[f, x], edge, f * wide + x + 2)
            for j, i in enumerate(dirs):
                sheet = put(sheet, pop[1, i, x], edge, (5 + j) * wide + x + 2)
            for k in range(2):
                sheet = put(sheet, field[k, x], inner, (10 + k) * wide + x + 2)
        sheets[side] = sheet


def join_kernel(nx, sheets, from_below, from_above, joined, rows_out):
    below, above = from_below[...], from_above[...]
    ny = below.shape[0]
    wide = nx + 4
    place = lax.rem(lanes(below.shape), wide)
    for side, shift in ((0, 0), (1, 2)):
        sheet = jnp.where(place < 2, roll(below, -shift, 1), sheets[side])
        sheet = jnp.where(place >= nx + 2, roll(above, shift, 1), sheet)
        joined[side] = sheet
        rows_out[side] = fold(sheet, ny)


def y_kernel(nx, field, pop, from_below, from_above, rows_out):
    psi, com, pair, low, high, _ = y_index(nx)
    below, above = (lambda f: from_below[f]), (lambda f: from_above[f])
    ny, nz = field.shape[2:]
    tile = lax.broadcasted_iota(jnp.int32, (8, nz), 0)
    for k in range(2):
        for x in range(nx):
            rows_out[psi(k, x)] = fold(field[k, x], ny)
        rows_out[psi(k, nx)], rows_out[psi(k, -1)] = fold(above(k), ny), fold(below(k), ny)
        rows_out[psi(k, nx + 1)], rows_out[psi(k, -2)] = fold(above(10 + k), ny), fold(below(10 + k), ny)
    for a in range(3):
        for x in range(nx):
            rows_out[com(a, x)] = fold(field[2 + a, x], ny)
        rows_out[com(a, nx)], rows_out[com(a, -1)] = fold(above(2 + a), ny), fold(below(2 + a), ny)
    for j, (plus, minus) in enumerate(YPAIR):
        for x in range(nx):
            rows_out[pair(j, x)] = jnp.where(tile < 4, pop[1, minus, x, 0:8], pop[1, plus, x, ny - 8 : ny])
    for where, source, step, dirs in ((low, below, 1, XP), (high, above, -1, XM)):
        plus, minus = dirs.index(VEL.index((step, 1, 0))) + 5, dirs.index(VEL.index((step, -1, 0))) + 5
        rows_out[where] = jnp.where(tile < 4, source(minus)[:8], source(plus)[ny - 8 :])


def merge_rows(from_y, n):
    if len(from_y) == 1:
        return from_y[0][n]
    below, above = from_y[0][n], from_y[1][n]
    return jnp.where(lax.broadcasted_iota(jnp.int32, above.shape, 0) < 4, above, below)


def z_kernel(y_parts, joined, *rest):
    from_y, (send_high, send_low) = rest[:y_parts], rest[y_parts:]
    for side, send in ((0, send_high), (1, send_low)):
        send[...] = jnp.concatenate([joined[side], merge_rows(from_y, side)], axis=0)


def store_rows(ref, at, main, halo):
    ny = main.shape[0]
    ref[(*at, slice(0, 8))] = halo
    ref[(*at, slice(8, 8 + ny))] = main
    ref[(*at, slice(8 + ny, 16 + ny))] = halo


def load_rows(ref, at, step, ny):
    main = ref[(*at, slice(8 + step, 8 + step + ny))]
    first = step if step >= 0 else 8 + ny + step
    return jnp.concatenate([main, ref[(*at, slice(first, first + 8))]], axis=0)


def posts(k, rho, vel, fluid, dirs, pop):
    out, made, parts = {}, {}, {}
    scaled = rho if TAU[k] == 1.0 else rho * (1.0 / TAU[k])
    square = vel[0] * vel[0] + vel[1] * vel[1] + vel[2] * vel[2]
    base = jnp.where(fluid, scaled - (1.5 * scaled) * square, BLOCKED)
    for weight in (W1, W2):
        parts[weight] = weight * base, (4.5 * weight) * scaled
    for i in dirs:
        whole, value = pop(i)
        cut = (lambda v: v) if whole else (lambda v: v[: value.shape[0]])
        if i == 0:
            equil = cut(base) * WEIGHT[0]
        else:
            lead = next(a for a in range(3) if VEL[i][a])
            main = i if VEL[i][lead] == 1 else OPP[i]
            if main not in made:
                along = None
                for a in range(3):
                    c = VEL[main][a]
                    if c:
                        u = cut(vel[a])
                        along = u if along is None else (along + u if c == 1 else along - u)
                share, factor = parts[WEIGHT[i]]
                flow = cut(factor) * along
                made[main] = cut(share) + flow * along, (2.0 / 3.0) * flow
            even, odd = made[main]
            equil = even + odd if main == i else even - odd
        out[i] = equil if TAU[k] == 1.0 else equil + (1.0 - 1.0 / TAU[k]) * value
    return out


def last_kernel(nx, y_parts, pop, solid, field, own_high, own_low, from_below, from_above, z_low, z_high, *rest):
    from_y, (out_hbm, out, a_ref, t_ref, dy_ref, dz_ref, zs_ref, gy_ref, gz_ref, post_ref, edge_ref, sems) = (
        rest[:y_parts],
        rest[y_parts:],
    )
    psi, com, pair, low, high, _ = y_index(nx)
    wide = nx + 4
    ny, nz = field.shape[2:]
    rows = lambda n: merge_rows(from_y, n)
    own_hi, own_lo, z_lo, z_hi = own_high[...], own_low[...], z_low[...], z_high[...]
    tall = (ny + 8, nz)
    lane = lanes(tall)

    def signed(k, x):
        if x < 0:
            main = from_below[k if x == -1 else 10 + k]
        elif x >= nx:
            main = from_above[k if x == nx else 10 + k]
        else:
            main = field[k, x]
        return jnp.concatenate([main, rows(psi(k, x))], axis=0)

    def shift_psi(k, x):
        at = (k, x + 2)
        a = jnp.abs(signed(k, x))
        column = k * wide + x + 2
        minus = jnp.where(lane == 0, jnp.abs(roll(z_lo, -column, 1)), roll(a, 1, 1))
        plus = jnp.where(lane == nz - 1, jnp.abs(roll(z_hi, nz - 1 - column, 1)), roll(a, -1, 1))
        z_sum, dz = plus + minus, plus - minus
        store_rows(a_ref, at, a[:ny], a[ny:])
        a_up, a_down = load_rows(a_ref, at, 1, ny), load_rows(a_ref, at, -1, ny)
        dy = a_up - a_down
        t_ref[at] = (a + a) + ((a_up + a_down) + z_sum)
        dy_ref[at] = dy
        dz_ref[at] = dz
        if -2 < x < nx + 1:
            store_rows(zs_ref, at, z_sum[:ny], z_sum[ny:])
            gy_ref[k, x + 1] = (dy + dy) + (load_rows(zs_ref, at, 1, ny) - load_rows(zs_ref, at, -1, ny))
            store_rows(a_ref, at, dz[:ny], dz[ny:])
            gz_ref[k, x + 1] = (dz + dz) + (load_rows(a_ref, at, 1, ny) + load_rows(a_ref, at, -1, ny))

    def speed(k, common, gradient):
        return [common[a] - (COUPLING * TAU[k] * W2) * gradient[a] for a in range(3)]

    def collide(k, x):
        n, other = x + 1, 1 - k
        gradient = (
            t_ref[other, n + 2] - t_ref[other, n],
            gy_ref[other, n] + (dy_ref[other, n + 2] + dy_ref[other, n]),
            gz_ref[other, n] + (dz_ref[other, n + 2] + dz_ref[other, n]),
        )
        common = []
        for a in range(3):
            main = from_below[2 + a] if x < 0 else from_above[2 + a] if x == nx else field[2 + a, x]
            common.append(jnp.concatenate([main, rows(com(a, x))], axis=0))
        own = signed(k, x)

        def population(i):
            if x < 0:
                main = from_below[5 + XP.index(i)]
            elif x == nx:
                main = from_above[5 + XM.index(i)]
            else:
                main = pop[1, i, x]
            if not VEL[i][1]:
                return False, main
            j = next(j for j, both in enumerate(YPAIR) if i in both)
            return True, jnp.concatenate([main, rows(low if x < 0 else high if x == nx else pair(j, x))], axis=0)

        dirs = XP if x < 0 else XM if x == nx else range(19)
        for i, value in posts(k, jnp.abs(own), speed(k, common, gradient), own > 0.0, dirs, population).items():
            if VEL[i][1]:
                store_rows(post_ref, (k, i, n), value[:ny], value[ny:])
            else:
                post_ref[k, i, n, 8 : 8 + ny] = value

    half = nz // 2

    def collide_sheets(k):
        is_low = lane < half
        part = lambda one, f, two, g: jnp.where(is_low, roll(one, -f * wide, 1), roll(two, half - g * wide, 1))
        right, left = (lambda v: roll(v, -1, 1)), (lambda v: roll(v, 1, 1))
        other = 1 - k
        own, a = part(z_lo, k, z_hi, k), jnp.abs(part(z_lo, other, z_hi, other))
        plus = jnp.abs(part(own_lo, other, own_hi, other))
        minus = jnp.abs(part(z_lo, 10 + other, z_hi, 10 + other))
        a_up, a_down = up(a), down(a)
        z_sum, dz, dy = plus + minus, plus - minus, a_up - a_down
        t = (a + a) + (a_up + a_down + z_sum)
        gradient = (
            right(t) - left(t),
            (dy + dy) + (up(z_sum) - down(z_sum) + right(dy) + left(dy)),
            (dz + dz) + (up(dz) + down(dz) + right(dz) + left(dz)),
        )
        common = [part(z_lo, 2 + a, z_hi, 2 + a) for a in range(3)]
        common[2] = jnp.where(is_low, common[2], -common[2])
        population = lambda i: (True, part(z_lo, 5 + ZP.index(i), z_hi, 5 + ZM.index(mirror(i))) if k else None)
        for i, value in posts(k, jnp.abs(own), speed(k, common, gradient), own > 0.0, ZP, population).items():
            edge_ref[k, ZP.index(i)] = roll(value, VEL[i][1], 0)[:ny]

    lane_of = lanes((ny, nz))

    def write(k, x):
        return pltpu.make_async_copy(out.at[k, :, x], out_hbm.at[k, :, x], sems.at[k, x])

    def finish(k, x):
        fluid = solid[x] == 0
        for i in range(19):
            cx, cy, cz = VEL[i]
            source = x - cx
            value = post_ref[k, i, source + 1, 8 - cy : 8 - cy + ny]
            if cz == 1:
                edge = roll(edge_ref[k, ZP.index(i)], -(source + 2), 1)
                value = jnp.where(lane_of == 0, edge, roll(value, 1, 1))
            elif cz == -1:
                edge = roll(edge_ref[k, ZP.index(mirror(i))], nz - 1 - half - (source + 2), 1)
                value = jnp.where(lane_of == nz - 1, edge, roll(value, -1, 1))
            if i:
                value = jnp.where(value < LIMIT, value, post_ref[k, OPP[i], x + 1, 8 : 8 + ny])
            out[k, i, x] = jnp.where(fluid, value, pop[k, i, x])
        write(k, x).start()

    for x in range(-2, 4):
        shift_psi(1, x)
    collide_sheets(0)
    for x in range(-1, 2):
        collide(0, x)
    later = [functools.partial(shift_psi, 0, x) for x in range(-2, nx + 2)]
    later += [functools.partial(collide_sheets, 1)] + [functools.partial(collide, 1, x) for x in range(-1, 2)]
    share = -(-len(later) // nx)
    for x in range(nx):
        if x + 4 < nx + 2:
            shift_psi(1, x + 4)
        if x + 2 < nx + 1:
            collide(0, x + 2)
        finish(0, x)
        for task in later[x * share : (x + 1) * share]:
            task()
    for x in range(nx):
        if x + 2 < nx + 1:
            collide(1, x + 2)
        finish(1, x)
    for k in range(2):
        for x in range(nx):
            write(k, x).wait()


def ring(value, axis, count, step):
    return lax.ppermute(value, axis, [(i, (i + step) % count) for i in range(count)])


def spread(high, low, axis, count):
    return ring(high, axis, count, 1), ring(low, axis, count, -1)


def spread_rows(rows, count):
    return spread(rows, rows, "gy", count) if count > 2 else (ring(rows, "gy", count, 1),)


def call(kernel, out_shape, *args, scratch=(), hbm_in=0, hbm_out=0, flops=200000, limit=16 * 2**20):
    space = lambda n, held: [pl.BlockSpec(memory_space=pltpu.HBM if j < held else pltpu.VMEM) for j in range(n)]
    args = [pltpu.with_memory_space_constraint(v, pltpu.HBM) if j < hbm_in else v for j, v in enumerate(args)]
    return pl.pallas_call(
        kernel,
        out_shape=[jax.ShapeDtypeStruct(*(s if isinstance(s[-1], type) else (s, jnp.float32))) for s in out_shape],
        in_specs=space(len(args), hbm_in),
        out_specs=space(len(out_shape), hbm_out),
        scratch_shapes=list(scratch),
        compiler_params=pltpu.CompilerParams(vmem_limit_bytes=limit),
        cost_estimate=pl.CostEstimate(flops=flops, bytes_accessed=flops, transcendentals=0),
    )(*args)


def body(sizes, pop, solid):
    return step(sizes, pop, solid)


def step(sizes, pop, solid):
    nx, ny, nz = solid.shape
    count = y_index(nx)[-1]
    wide = nx + 4
    face, plane, tall, padded = (HALO, ny, nz), (ny, nz), (ny + 8, nz), (ny + 16, nz)
    gx, gy, gz = sizes["gx"], sizes["gy"], sizes["gz"]
    y_parts = 1 if gy == 2 else 2
    field, face_high, face_low, rim_high, rim_low, pop_v, solid_v = call(
        first_kernel,
        [(5, nx, ny, nz), face, face, plane, plane, pop.shape, (solid.shape, jnp.int32)],
        pop, solid,
        scratch=[pltpu.SemaphoreType.DMA((nx + 1,))],
        hbm_in=2,
    )
    rims = spread(rim_high, rim_low, "gx", gx)
    faces = spread(face_high, face_low, "gx", gx)
    (sheets,) = call(column_kernel, [(2,) + plane], field, pop_v)
    joined, ends = call(functools.partial(join_kernel, nx), [(2,) + plane, (2, 8, nz)], sheets, *rims)
    ends = spread_rows(ends, gy)
    own = call(functools.partial(z_kernel, y_parts), [tall, tall], joined, *ends)
    far = spread(*own, "gz", gz)
    (rows,) = call(functools.partial(y_kernel, nx), [(count, 8, nz)], field, pop_v, *faces)
    from_y = spread_rows(rows, gy)
    vmem = lambda *s: pltpu.VMEM(s, jnp.float32)
    (result,) = call(
        functools.partial(last_kernel, nx, y_parts),
        [pop.shape],
        pop_v, solid_v, field, *own, *faces, *far, *from_y,
        scratch=[vmem(*pop.shape), vmem(2, wide, *padded)]
        + [vmem(2, wide, *tall)] * 3
        + [vmem(2, wide, *padded)]
        + [vmem(2, nx + 2, *tall)] * 2
        + [vmem(2, 19, nx + 2, *padded), vmem(2, 5, ny, nz), pltpu.SemaphoreType.DMA((2, nx))],
        hbm_out=1,
    )
    return result


def solution(mesh):
    sizes = dict(mesh.shape)
    spec = P(None, None, "gx", "gy", "gz")
    return jax.shard_map(
        functools.partial(body, sizes),
        mesh=mesh,
        in_specs=(spec, P("gx", "gy", "gz")),
        out_specs=spec,
        check_vma=False,
    )
```

```python
import functools

import jax
import jax.numpy as jnp
from jax import lax
from jax.experimental import pallas as pl
from jax.experimental.pallas import tpu as pltpu
from jax.sharding import PartitionSpec as P


VEL = [
    (0, 0, 0),
    (1, 0, 0), (-1, 0, 0), (0, 1, 0), (0, -1, 0), (0, 0, 1), (0, 0, -1),
    (1, 1, 0), (-1, -1, 0), (1, -1, 0), (-1, 1, 0),
    (1, 0, 1), (-1, 0, -1), (1, 0, -1), (-1, 0, 1),
    (0, 1, 1), (0, -1, -1), (0, 1, -1), (0, -1, 1),
]
WEIGHT = [1.0 / 3.0] + [1.0 / 18.0] * 6 + [1.0 / 36.0] * 12
OPP = [0, 2, 1, 4, 3, 6, 5, 8, 7, 10, 9, 12, 11, 14, 13, 16, 15, 18, 17]
COUPLING = 0.9
TAU = (1.0, 0.8)
WALL = (0.3, 1.5)
W1, W2 = 1.0 / 18.0, 1.0 / 36.0
BLOCKED = 1e32
LIMIT = 1e29

XP = [i for i in range(19) if VEL[i][0] == 1]
XM = [i for i in range(19) if VEL[i][0] == -1]
ZP = [i for i in range(19) if VEL[i][2] == 1]
ZM = [i for i in range(19) if VEL[i][2] == -1]
YP = [i for i in range(19) if VEL[i][1] == 1]
YPAIR = [(i, VEL.index((VEL[i][0], -1, VEL[i][2]))) for i in YP]


def mirror(i):
    return VEL.index((VEL[i][0], VEL[i][1], -VEL[i][2]))


HALO = 12


def lanes(shape):
    return lax.broadcasted_iota(jnp.int32, shape, len(shape) - 1)


def roll(v, shift, axis):
    shift = shift % v.shape[axis]
    return pltpu.roll(v, shift, axis) if shift else v


def up(v):
    return roll(v, -1, 0)


def down(v):
    return roll(v, 1, 0)


def fold(v, rows):
    tile = lax.broadcasted_iota(jnp.int32, (8, v.shape[1]), 0)
    return jnp.where(tile < 4, v[:8], v[rows - 8 : rows])


def put(sheet, value, source, target):
    return jnp.where(lanes(sheet.shape) == target, roll(value, target - source, 1), sheet)


def y_index(nx):
    wide, mid = nx + 4, nx + 2
    psi = lambda k, x: k * wide + x + 2
    com = lambda a, x: 2 * wide + a * mid + x + 1
    base = 2 * wide + 3 * mid
    pair = lambda j, x: base + j * nx + x
    low, high = base + 5 * nx, base + 5 * nx + 1
    return psi, com, pair, low, high, high + 1


def first_kernel(pop_hbm, solid_hbm, field, face_high, face_low, rim_high, rim_low, pop, solid, sems):
    nx, ny, nz = solid_hbm.shape
    wide = nx + 4

    def face_side(step, dirs, edge, inner, face_out, rim_out):
        face = [field[f, edge] for f in range(5)] + [pop[1, i, edge] for i in dirs] + [field[f, inner] for f in range(2)]
        rim = jnp.zeros((ny, nz), jnp.float32)
        for cz, z_dirs, z_edge, z_inner in ((1, ZP, nz - 1, nz - 2), (-1, ZM, 0, 1)):
            near, far = rim_lanes(wide, step, cz)
            for k in range(2):
                for f, lane in ((k, z_edge), (10 + k, z_inner)):
                    rim = put(rim, face[k], lane, f * wide + near)
                    rim = put(rim, face[10 + k], lane, f * wide + far)
            for a in range(3):
                rim = put(rim, face[2 + a], z_edge, (2 + a) * wide + near)
            i = VEL.index((step, 0, cz))
            rim = put(rim, face[5 + dirs.index(i)], z_edge, (5 + z_dirs.index(i)) * wide + near)
        for f in range(HALO):
            face_out[f] = face[f]
        rim_out[...] = rim

    flag_copy = pltpu.make_async_copy(solid_hbm, solid, sems.at[nx])
    copies = [pltpu.make_async_copy(pop_hbm.at[:, :, x], pop.at[:, :, x], sems.at[x]) for x in range(nx)]
    flag_copy.start()
    for x in range(nx):
        copies[x].start()
    flag_copy.wait()
    for x in range(nx):
        copies[x].wait()
        fluid = solid[x] == 0
        q = []
        rho0 = rho1 = None
        for i in range(19):
            p0, p1 = pop[0, i, x], pop[1, i, x]
            rho0 = p0 if rho0 is None else rho0 + p0
            rho1 = p1 if rho1 is None else rho1 + p1
            q.append(p0 * (1.0 / TAU[0]) + p1 * (1.0 / TAU[1]))
        inverse = 1.0 / (rho0 * (1.0 / TAU[0]) + rho1 * (1.0 / TAU[1]))
        field[0, x] = jnp.where(fluid, rho0, -WALL[0])
        field[1, x] = jnp.where(fluid, rho1, -WALL[1])
        for a in range(3):
            total = None
            for i in range(1, 19):
                if VEL[i][a] == 1:
                    term = q[i] - q[OPP[i]]
                    total = term if total is None else total + term
            field[2 + a, x] = total * inverse
        if x == 1:
            face_side(-1, XM, 0, 1, face_low, rim_low)
    face_side(1, XP, nx - 1, nx - 2, face_high, rim_high)


def rim_lanes(wide, step, cz):
    if step == 1:
        return (1, 0) if cz == 1 else (3, 2)
    return (wide - 2, wide - 1) if cz == 1 else (wide - 4, wide - 3)


def column_kernel(field, pop, sheets):
    nx, ny, nz = field.shape[1:]
    wide = nx + 4
    for side, edge, inner, dirs in ((0, nz - 1, nz - 2, ZP), (1, 0, 1, ZM)):
        sheet = jnp.zeros((ny, nz), jnp.float32)
        for x in range(nx):
            for f in range(5):
                sheet = put(sheet, field[f, x], edge, f * wide + x + 2)
            for j, i in enumerate(dirs):
                sheet = put(sheet, pop[1, i, x], edge, (5 + j) * wide + x + 2)
            for k in range(2):
                sheet = put(sheet, field[k, x], inner, (10 + k) * wide + x + 2)
        sheets[side] = sheet


def join_kernel(nx, sheets, from_below, from_above, joined, rows_out):
    below, above = from_below[...], from_above[...]
    ny = below.shape[0]
    wide = nx + 4
    place = lax.rem(lanes(below.shape), wide)
    for side, shift in ((0, 0), (1, 2)):
        sheet = jnp.where(place < 2, roll(below, -shift, 1), sheets[side])
        sheet = jnp.where(place >= nx + 2, roll(above, shift, 1), sheet)
        joined[side] = sheet
        rows_out[side] = fold(sheet, ny)


def y_kernel(nx, field, pop, from_below, from_above, rows_out):
    psi, com, pair, low, high, _ = y_index(nx)
    below, above = (lambda f: from_below[f]), (lambda f: from_above[f])
    ny, nz = field.shape[2:]
    tile = lax.broadcasted_iota(jnp.int32, (8, nz), 0)
    for k in range(2):
        for x in range(nx):
            rows_out[psi(k, x)] = fold(field[k, x], ny)
        rows_out[psi(k, nx)], rows_out[psi(k, -1)] = fold(above(k), ny), fold(below(k), ny)
        rows_out[psi(k, nx + 1)], rows_out[psi(k, -2)] = fold(above(10 + k), ny), fold(below(10 + k), ny)
    for a in range(3):
        for x in range(nx):
            rows_out[com(a, x)] = fold(field[2 + a, x], ny)
        rows_out[com(a, nx)], rows_out[com(a, -1)] = fold(above(2 + a), ny), fold(below(2 + a), ny)
    for j, (plus, minus) in enumerate(YPAIR):
        for x in range(nx):
            rows_out[pair(j, x)] = jnp.where(tile < 4, pop[1, minus, x, 0:8], pop[1, plus, x, ny - 8 : ny])
    for where, source, step, dirs in ((low, below, 1, XP), (high, above, -1, XM)):
        plus, minus = dirs.index(VEL.index((step, 1, 0))) + 5, dirs.index(VEL.index((step, -1, 0))) + 5
        rows_out[where] = jnp.where(tile < 4, source(minus)[:8], source(plus)[ny - 8 :])


def merge_rows(from_y, n):
    if len(from_y) == 1:
        return from_y[0][n]
    below, above = from_y[0][n], from_y[1][n]
    return jnp.where(lax.broadcasted_iota(jnp.int32, above.shape, 0) < 4, above, below)


def z_kernel(y_parts, joined, *rest):
    from_y, (send_high, send_low) = rest[:y_parts], rest[y_parts:]
    for side, send in ((0, send_high), (1, send_low)):
        send[...] = jnp.concatenate([joined[side], merge_rows(from_y, side)], axis=0)


def store_rows(ref, at, main, halo):
    ny = main.shape[0]
    ref[(*at, slice(0, 8))] = halo
    ref[(*at, slice(8, 8 + ny))] = main
    ref[(*at, slice(8 + ny, 16 + ny))] = halo


def load_rows(ref, at, step, ny):
    main = ref[(*at, slice(8 + step, 8 + step + ny))]
    first = step if step >= 0 else 8 + ny + step
    return jnp.concatenate([main, ref[(*at, slice(first, first + 8))]], axis=0)


def posts(k, rho, vel, fluid, dirs, pop):
    out, made, parts = {}, {}, {}
    scaled = rho if TAU[k] == 1.0 else rho * (1.0 / TAU[k])
    square = vel[0] * vel[0] + vel[1] * vel[1] + vel[2] * vel[2]
    base = jnp.where(fluid, scaled - (1.5 * scaled) * square, BLOCKED)
    for weight in (W1, W2):
        parts[weight] = weight * base, (4.5 * weight) * scaled
    for i in dirs:
        whole, value = pop(i)
        cut = (lambda v: v) if whole else (lambda v: v[: value.shape[0]])
        if i == 0:
            equil = cut(base) * WEIGHT[0]
        else:
            lead = next(a for a in range(3) if VEL[i][a])
            main = i if VEL[i][lead] == 1 else OPP[i]
            if main not in made:
                along = None
                for a in range(3):
                    c = VEL[main][a]
                    if c:
                        u = cut(vel[a])
                        along = u if along is None else (along + u if c == 1 else along - u)
                share, factor = parts[WEIGHT[i]]
                flow = cut(factor) * along
                made[main] = cut(share) + flow * along, (2.0 / 3.0) * flow
            even, odd = made[main]
            equil = even + odd if main == i else even - odd
        out[i] = equil if TAU[k] == 1.0 else equil + (1.0 - 1.0 / TAU[k]) * value
    return out


def last_kernel(nx, y_parts, pop, solid, field, own_high, own_low, from_below, from_above, z_low, z_high, *rest):
    from_y, (out_hbm, out, a_ref, t_ref, dy_ref, dz_ref, zs_ref, gy_ref, gz_ref, post_ref, edge_ref, sems) = (
        rest[:y_parts],
        rest[y_parts:],
    )
    psi, com, pair, low, high, _ = y_index(nx)
    wide = nx + 4
    ny, nz = field.shape[2:]
    rows = lambda n: merge_rows(from_y, n)
    own_hi, own_lo, z_lo, z_hi = own_high[...], own_low[...], z_low[...], z_high[...]
    tall = (ny + 8, nz)
    lane = lanes(tall)

    def signed(k, x):
        if x < 0:
            main = from_below[k if x == -1 else 10 + k]
        elif x >= nx:
            main = from_above[k if x == nx else 10 + k]
        else:
            main = field[k, x]
        return jnp.concatenate([main, rows(psi(k, x))], axis=0)

    def shift_psi(k, x):
        at = (k, x + 2)
        a = jnp.abs(signed(k, x))
        column = k * wide + x + 2
        minus = jnp.where(lane == 0, jnp.abs(roll(z_lo, -column, 1)), roll(a, 1, 1))
        plus = jnp.where(lane == nz - 1, jnp.abs(roll(z_hi, nz - 1 - column, 1)), roll(a, -1, 1))
        z_sum, dz = plus + minus, plus - minus
        store_rows(a_ref, at, a[:ny], a[ny:])
        a_up, a_down = load_rows(a_ref, at, 1, ny), load_rows(a_ref, at, -1, ny)
        dy = a_up - a_down
        t_ref[at] = (a + a) + ((a_up + a_down) + z_sum)
        dy_ref[at] = dy
        dz_ref[at] = dz
        if -2 < x < nx + 1:
            store_rows(zs_ref, at, z_sum[:ny], z_sum[ny:])
            gy_ref[k, x + 1] = (dy + dy) + (load_rows(zs_ref, at, 1, ny) - load_rows(zs_ref, at, -1, ny))
            store_rows(a_ref, at, dz[:ny], dz[ny:])
            gz_ref[k, x + 1] = (dz + dz) + (load_rows(a_ref, at, 1, ny) + load_rows(a_ref, at, -1, ny))

    def speed(k, common, gradient):
        return [common[a] - (COUPLING * TAU[k] * W2) * gradient[a] for a in range(3)]

    def collide(k, x):
        n, other = x + 1, 1 - k
        gradient = (
            t_ref[other, n + 2] - t_ref[other, n],
            gy_ref[other, n] + (dy_ref[other, n + 2] + dy_ref[other, n]),
            gz_ref[other, n] + (dz_ref[other, n + 2] + dz_ref[other, n]),
        )
        common = []
        for a in range(3):
            main = from_below[2 + a] if x < 0 else from_above[2 + a] if x == nx else field[2 + a, x]
            common.append(jnp.concatenate([main, rows(com(a, x))], axis=0))
        own = signed(k, x)

        def population(i):
            if x < 0:
                main = from_below[5 + XP.index(i)]
            elif x == nx:
                main = from_above[5 + XM.index(i)]
            else:
                main = pop[1, i, x]
            if not VEL[i][1]:
                return False, main
            j = next(j for j, both in enumerate(YPAIR) if i in both)
            return True, jnp.concatenate([main, rows(low if x < 0 else high if x == nx else pair(j, x))], axis=0)

        dirs = XP if x < 0 else XM if x == nx else range(19)
        for i, value in posts(k, jnp.abs(own), speed(k, common, gradient), own > 0.0, dirs, population).items():
            if VEL[i][1]:
                store_rows(post_ref, (k, i, n), value[:ny], value[ny:])
            else:
                post_ref[k, i, n, 8 : 8 + ny] = value

    half = nz // 2

    def collide_sheets(k):
        is_low = lane < half
        part = lambda one, f, two, g: jnp.where(is_low, roll(one, -f * wide, 1), roll(two, half - g * wide, 1))
        right, left = (lambda v: roll(v, -1, 1)), (lambda v: roll(v, 1, 1))
        other = 1 - k
        own, a = part(z_lo, k, z_hi, k), jnp.abs(part(z_lo, other, z_hi, other))
        plus = jnp.abs(part(own_lo, other, own_hi, other))
        minus = jnp.abs(part(z_lo, 10 + other, z_hi, 10 + other))
        a_up, a_down = up(a), down(a)
        z_sum, dz, dy = plus + minus, plus - minus, a_up - a_down
        t = (a + a) + (a_up + a_down + z_sum)
        gradient = (
            right(t) - left(t),
            (dy + dy) + (up(z_sum) - down(z_sum) + right(dy) + left(dy)),
            (dz + dz) + (up(dz) + down(dz) + right(dz) + left(dz)),
        )
        common = [part(z_lo, 2 + a, z_hi, 2 + a) for a in range(3)]
        common[2] = jnp.where(is_low, common[2], -common[2])
        population = lambda i: (True, part(z_lo, 5 + ZP.index(i), z_hi, 5 + ZM.index(mirror(i))) if k else None)
        for i, value in posts(k, jnp.abs(own), speed(k, common, gradient), own > 0.0, ZP, population).items():
            edge_ref[k, ZP.index(i)] = roll(value, VEL[i][1], 0)[:ny]

    lane_of = lanes((ny, nz))

    def write(k, x):
        cut = (k, slice(None), slice(x - x % 2, min(x - x % 2 + 2, nx)))
        return pltpu.make_async_copy(out.at[cut], out_hbm.at[cut], sems.at[k, x])

    def finish(k, x):
        fluid = solid[x] == 0
        for i in range(19):
            cx, cy, cz = VEL[i]
            source = x - cx
            value = post_ref[k, i, source + 1, 8 - cy : 8 - cy + ny]
            if cz == 1:
                edge = roll(edge_ref[k, ZP.index(i)], -(source + 2), 1)
                value = jnp.where(lane_of == 0, edge, roll(value, 1, 1))
            elif cz == -1:
                edge = roll(edge_ref[k, ZP.index(mirror(i))], nz - 1 - half - (source + 2), 1)
                value = jnp.where(lane_of == nz - 1, edge, roll(value, -1, 1))
            if i:
                value = jnp.where(value < LIMIT, value, post_ref[k, OPP[i], x + 1, 8 : 8 + ny])
            out[k, i, x] = jnp.where(fluid, value, pop[k, i, x])
        if x % 2 or x == nx - 1:
            write(k, x).start()

    for x in range(-2, 4):
        shift_psi(1, x)
    collide_sheets(0)
    for x in range(-1, 2):
        collide(0, x)
    later = [functools.partial(shift_psi, 0, x) for x in range(-2, nx + 2)]
    later += [functools.partial(collide_sheets, 1)] + [functools.partial(collide, 1, x) for x in range(-1, 2)]
    share = -(-len(later) // nx)
    for x in range(nx):
        if x + 4 < nx + 2:
            shift_psi(1, x + 4)
        if x + 2 < nx + 1:
            collide(0, x + 2)
        finish(0, x)
        for task in later[x * share : (x + 1) * share]:
            task()
    for x in range(nx):
        if x + 2 < nx + 1:
            collide(1, x + 2)
        finish(1, x)
    for k in range(2):
        for x in range(nx):
            if x % 2 or x == nx - 1:
                write(k, x).wait()


def ring(value, axis, count, step):
    return lax.ppermute(value, axis, [(i, (i + step) % count) for i in range(count)])


def spread(high, low, axis, count):
    return ring(high, axis, count, 1), ring(low, axis, count, -1)


def spread_rows(rows, count):
    return spread(rows, rows, "gy", count) if count > 2 else (ring(rows, "gy", count, 1),)


def call(kernel, out_shape, *args, scratch=(), hbm_in=0, hbm_out=0, flops=200000, limit=16 * 2**20):
    space = lambda n, held: [pl.BlockSpec(memory_space=pltpu.HBM if j < held else pltpu.VMEM) for j in range(n)]
    args = [pltpu.with_memory_space_constraint(v, pltpu.HBM) if j < hbm_in else v for j, v in enumerate(args)]
    return pl.pallas_call(
        kernel,
        out_shape=[jax.ShapeDtypeStruct(*(s if isinstance(s[-1], type) else (s, jnp.float32))) for s in out_shape],
        in_specs=space(len(args), hbm_in),
        out_specs=space(len(out_shape), hbm_out),
        scratch_shapes=list(scratch),
        compiler_params=pltpu.CompilerParams(vmem_limit_bytes=limit),
        cost_estimate=pl.CostEstimate(flops=flops, bytes_accessed=flops, transcendentals=0),
    )(*args)


def body(sizes, pop, solid):
    return step(sizes, pop, solid)


def step(sizes, pop, solid):
    nx, ny, nz = solid.shape
    count = y_index(nx)[-1]
    wide = nx + 4
    face, plane, tall, padded = (HALO, ny, nz), (ny, nz), (ny + 8, nz), (ny + 16, nz)
    gx, gy, gz = sizes["gx"], sizes["gy"], sizes["gz"]
    y_parts = 1 if gy == 2 else 2
    field, face_high, face_low, rim_high, rim_low, pop_v, solid_v = call(
        first_kernel,
        [(5, nx, ny, nz), face, face, plane, plane, pop.shape, (solid.shape, jnp.int32)],
        pop, solid,
        scratch=[pltpu.SemaphoreType.DMA((nx + 1,))],
        hbm_in=2,
    )
    rims = spread(rim_high, rim_low, "gx", gx)
    faces = spread(face_high, face_low, "gx", gx)
    (sheets,) = call(column_kernel, [(2,) + plane], field, pop_v)
    joined, ends = call(functools.partial(join_kernel, nx), [(2,) + plane, (2, 8, nz)], sheets, *rims)
    ends = spread_rows(ends, gy)
    own = call(functools.partial(z_kernel, y_parts), [tall, tall], joined, *ends)
    far = spread(*own, "gz", gz)
    (rows,) = call(functools.partial(y_kernel, nx), [(count, 8, nz)], field, pop_v, *faces)
    from_y = spread_rows(rows, gy)
    vmem = lambda *s: pltpu.VMEM(s, jnp.float32)
    (result,) = call(
        functools.partial(last_kernel, nx, y_parts),
        [pop.shape],
        pop_v, solid_v, field, *own, *faces, *far, *from_y,
        scratch=[vmem(*pop.shape), vmem(2, wide, *padded)]
        + [vmem(2, wide, *tall)] * 3
        + [vmem(2, wide, *padded)]
        + [vmem(2, nx + 2, *tall)] * 2
        + [vmem(2, 19, nx + 2, *padded), vmem(2, 5, ny, nz), pltpu.SemaphoreType.DMA((2, nx))],
        hbm_out=1,
    )
    return result


def solution(mesh):
    sizes = dict(mesh.shape)
    spec = P(None, None, "gx", "gy", "gz")
    return jax.shard_map(
        functools.partial(body, sizes),
        mesh=mesh,
        in_specs=(spec, P("gx", "gy", "gz")),
        out_specs=spec,
        check_vma=False,
    )
```

```python
import functools

import jax
import jax.numpy as jnp
from jax import lax
from jax.experimental import pallas as pl
from jax.experimental.pallas import tpu as pltpu
from jax.sharding import PartitionSpec as P


VEL = [
    (0, 0, 0),
    (1, 0, 0), (-1, 0, 0), (0, 1, 0), (0, -1, 0), (0, 0, 1), (0, 0, -1),
    (1, 1, 0), (-1, -1, 0), (1, -1, 0), (-1, 1, 0),
    (1, 0, 1), (-1, 0, -1), (1, 0, -1), (-1, 0, 1),
    (0, 1, 1), (0, -1, -1), (0, 1, -1), (0, -1, 1),
]
WEIGHT = [1.0 / 3.0] + [1.0 / 18.0] * 6 + [1.0 / 36.0] * 12
OPP = [0, 2, 1, 4, 3, 6, 5, 8, 7, 10, 9, 12, 11, 14, 13, 16, 15, 18, 17]
COUPLING = 0.9
TAU = (1.0, 0.8)
WALL = (0.3, 1.5)
W1, W2 = 1.0 / 18.0, 1.0 / 36.0
BLOCKED = 1e32
LIMIT = 1e29

XP = [i for i in range(19) if VEL[i][0] == 1]
XM = [i for i in range(19) if VEL[i][0] == -1]
ZP = [i for i in range(19) if VEL[i][2] == 1]
ZM = [i for i in range(19) if VEL[i][2] == -1]
YP = [i for i in range(19) if VEL[i][1] == 1]
YPAIR = [(i, VEL.index((VEL[i][0], -1, VEL[i][2]))) for i in YP]


def mirror(i):
    return VEL.index((VEL[i][0], VEL[i][1], -VEL[i][2]))


HALO = 12


def lanes(shape):
    return lax.broadcasted_iota(jnp.int32, shape, len(shape) - 1)


def roll(v, shift, axis):
    shift = shift % v.shape[axis]
    return pltpu.roll(v, shift, axis) if shift else v


def up(v):
    return roll(v, -1, 0)


def down(v):
    return roll(v, 1, 0)


def fold(v, rows):
    tile = lax.broadcasted_iota(jnp.int32, (8, v.shape[1]), 0)
    return jnp.where(tile < 4, v[:8], v[rows - 8 : rows])


def put(sheet, value, source, target):
    return jnp.where(lanes(sheet.shape) == target, roll(value, target - source, 1), sheet)


def y_index(nx):
    wide, mid = nx + 4, nx + 2
    psi = lambda k, x: k * wide + x + 2
    com = lambda a, x: 2 * wide + a * mid + x + 1
    base = 2 * wide + 3 * mid
    pair = lambda j, x: base + j * nx + x
    low, high = base + 5 * nx, base + 5 * nx + 1
    return psi, com, pair, low, high, high + 1


def first_kernel(pop_hbm, solid_hbm, field, face_high, face_low, rim_high, rim_low, pop, solid, sems):
    nx, ny, nz = solid_hbm.shape
    wide = nx + 4

    def face_side(step, dirs, edge, inner, face_out, rim_out):
        face = [field[f, edge] for f in range(5)] + [pop[1, i, edge] for i in dirs] + [field[f, inner] for f in range(2)]
        rim = jnp.zeros((ny, nz), jnp.float32)
        for cz, z_dirs, z_edge, z_inner in ((1, ZP, nz - 1, nz - 2), (-1, ZM, 0, 1)):
            near, far = rim_lanes(wide, step, cz)
            for k in range(2):
                for f, lane in ((k, z_edge), (10 + k, z_inner)):
                    rim = put(rim, face[k], lane, f * wide + near)
                    rim = put(rim, face[10 + k], lane, f * wide + far)
            for a in range(3):
                rim = put(rim, face[2 + a], z_edge, (2 + a) * wide + near)
            i = VEL.index((step, 0, cz))
            rim = put(rim, face[5 + dirs.index(i)], z_edge, (5 + z_dirs.index(i)) * wide + near)
        for f in range(HALO):
            face_out[f] = face[f]
        rim_out[...] = rim

    flag_copy = pltpu.make_async_copy(solid_hbm, solid, sems.at[nx])
    copies = [pltpu.make_async_copy(pop_hbm.at[:, :, x], pop.at[:, :, x], sems.at[x]) for x in range(nx)]
    flag_copy.start()
    for x in range(nx):
        copies[x].start()
    flag_copy.wait()
    for x in range(nx):
        copies[x].wait()
        fluid = solid[x] == 0
        q = []
        rho0 = rho1 = None
        for i in range(19):
            p0, p1 = pop[0, i, x], pop[1, i, x]
            rho0 = p0 if rho0 is None else rho0 + p0
            rho1 = p1 if rho1 is None else rho1 + p1
            q.append(p0 * (1.0 / TAU[0]) + p1 * (1.0 / TAU[1]))
        inverse = 1.0 / (rho0 * (1.0 / TAU[0]) + rho1 * (1.0 / TAU[1]))
        field[0, x] = jnp.where(fluid, rho0, -WALL[0])
        field[1, x] = jnp.where(fluid, rho1, -WALL[1])
        for a in range(3):
            total = None
            for i in range(1, 19):
                if VEL[i][a] == 1:
                    term = q[i] - q[OPP[i]]
                    total = term if total is None else total + term
            field[2 + a, x] = total * inverse
        if x == 1:
            face_side(-1, XM, 0, 1, face_low, rim_low)
    face_side(1, XP, nx - 1, nx - 2, face_high, rim_high)


def rim_lanes(wide, step, cz):
    if step == 1:
        return (1, 0) if cz == 1 else (3, 2)
    return (wide - 2, wide - 1) if cz == 1 else (wide - 4, wide - 3)


def column_kernel(field, pop, sheets):
    nx, ny, nz = field.shape[1:]
    wide = nx + 4
    for side, edge, inner, dirs in ((0, nz - 1, nz - 2, ZP), (1, 0, 1, ZM)):
        sheet = jnp.zeros((ny, nz), jnp.float32)
        for x in range(nx):
            for f in range(5):
                sheet = put(sheet, field[f, x], edge, f * wide + x + 2)
            for j, i in enumerate(dirs):
                sheet = put(sheet, pop[1, i, x], edge, (5 + j) * wide + x + 2)
            for k in range(2):
                sheet = put(sheet, field[k, x], inner, (10 + k) * wide + x + 2)
        sheets[side] = sheet


def join_kernel(nx, sheets, from_below, from_above, joined, rows_out):
    below, above = from_below[...], from_above[...]
    ny = below.shape[0]
    wide = nx + 4
    place = lax.rem(lanes(below.shape), wide)
    for side, shift in ((0, 0), (1, 2)):
        sheet = jnp.where(place < 2, roll(below, -shift, 1), sheets[side])
        sheet = jnp.where(place >= nx + 2, roll(above, shift, 1), sheet)
        joined[side] = sheet
        rows_out[side] = fold(sheet, ny)


def y_kernel(nx, field, pop, from_below, from_above, rows_out):
    psi, com, pair, low, high, _ = y_index(nx)
    below, above = (lambda f: from_below[f]), (lambda f: from_above[f])
    ny, nz = field.shape[2:]
    tile = lax.broadcasted_iota(jnp.int32, (8, nz), 0)
    for k in range(2):
        for x in range(nx):
            rows_out[psi(k, x)] = fold(field[k, x], ny)
        rows_out[psi(k, nx)], rows_out[psi(k, -1)] = fold(above(k), ny), fold(below(k), ny)
        rows_out[psi(k, nx + 1)], rows_out[psi(k, -2)] = fold(above(10 + k), ny), fold(below(10 + k), ny)
    for a in range(3):
        for x in range(nx):
            rows_out[com(a, x)] = fold(field[2 + a, x], ny)
        rows_out[com(a, nx)], rows_out[com(a, -1)] = fold(above(2 + a), ny), fold(below(2 + a), ny)
    for j, (plus, minus) in enumerate(YPAIR):
        for x in range(nx):
            rows_out[pair(j, x)] = jnp.where(tile < 4, pop[1, minus, x, 0:8], pop[1, plus, x, ny - 8 : ny])
    for where, source, step, dirs in ((low, below, 1, XP), (high, above, -1, XM)):
        plus, minus = dirs.index(VEL.index((step, 1, 0))) + 5, dirs.index(VEL.index((step, -1, 0))) + 5
        rows_out[where] = jnp.where(tile < 4, source(minus)[:8], source(plus)[ny - 8 :])


def merge_rows(from_y, n):
    if len(from_y) == 1:
        return from_y[0][n]
    below, above = from_y[0][n], from_y[1][n]
    return jnp.where(lax.broadcasted_iota(jnp.int32, above.shape, 0) < 4, above, below)


def z_kernel(y_parts, joined, *rest):
    from_y, (send_high, send_low) = rest[:y_parts], rest[y_parts:]
    for side, send in ((0, send_high), (1, send_low)):
        send[...] = jnp.concatenate([joined[side], merge_rows(from_y, side)], axis=0)


def store_rows(ref, at, main, halo):
    ny = main.shape[0]
    ref[(*at, slice(0, 8))] = halo
    ref[(*at, slice(8, 8 + ny))] = main
    ref[(*at, slice(8 + ny, 16 + ny))] = halo


def load_rows(ref, at, step, ny):
    main = ref[(*at, slice(8 + step, 8 + step + ny))]
    first = step if step >= 0 else 8 + ny + step
    return jnp.concatenate([main, ref[(*at, slice(first, first + 8))]], axis=0)


def posts(k, rho, vel, fluid, dirs, pop):
    out, made, parts = {}, {}, {}
    scaled = rho if TAU[k] == 1.0 else rho * (1.0 / TAU[k])
    square = vel[0] * vel[0] + vel[1] * vel[1] + vel[2] * vel[2]
    base = jnp.where(fluid, scaled - (1.5 * scaled) * square, BLOCKED)
    for weight in (W1, W2):
        parts[weight] = weight * base, (4.5 * weight) * scaled
    for i in dirs:
        whole, value = pop(i)
        cut = (lambda v: v) if whole else (lambda v: v[: value.shape[0]])
        if i == 0:
            equil = cut(base) * WEIGHT[0]
        else:
            lead = next(a for a in range(3) if VEL[i][a])
            main = i if VEL[i][lead] == 1 else OPP[i]
            if main not in made:
                along = None
                for a in range(3):
                    c = VEL[main][a]
                    if c:
                        u = cut(vel[a])
                        along = u if along is None else (along + u if c == 1 else along - u)
                share, factor = parts[WEIGHT[i]]
                flow = cut(factor) * along
                made[main] = cut(share) + flow * along, (2.0 / 3.0) * flow
            even, odd = made[main]
            equil = even + odd if main == i else even - odd
        out[i] = equil if TAU[k] == 1.0 else equil + (1.0 - 1.0 / TAU[k]) * value
    return out


def last_kernel(nx, y_parts, pop, solid, field, own_high, own_low, from_below, from_above, z_low, z_high, *rest):
    from_y, (out_hbm, out, a_ref, t_ref, dy_ref, dz_ref, zs_ref, gy_ref, gz_ref, post_ref, edge_ref, sems) = (
        rest[:y_parts],
        rest[y_parts:],
    )
    psi, com, pair, low, high, _ = y_index(nx)
    wide = nx + 4
    ny, nz = field.shape[2:]
    rows = lambda n: merge_rows(from_y, n)
    own_hi, own_lo, z_lo, z_hi = own_high[...], own_low[...], z_low[...], z_high[...]
    tall = (ny + 8, nz)
    lane = lanes(tall)

    def pairs(low, high, shape):
        is_even, high = lanes(shape) % 2 == 0, roll(high, -1, 1)
        return jnp.where(is_even, low, high), jnp.where(is_even, high, low)

    beyond = pairs(z_lo, z_hi, tall)

    def signed(k, x):
        if x < 0:
            main = from_below[k if x == -1 else 10 + k]
        elif x >= nx:
            main = from_above[k if x == nx else 10 + k]
        else:
            main = field[k, x]
        return jnp.concatenate([main, rows(psi(k, x))], axis=0)

    def shift_psi(k, x):
        at = (k, x + 2)
        a = jnp.abs(signed(k, x))
        column = k * wide + x + 2
        outer = jnp.abs(roll(beyond[column % 2], -column, 1))
        minus = jnp.where(lane == 0, outer, roll(a, 1, 1))
        plus = jnp.where(lane == nz - 1, outer, roll(a, -1, 1))
        z_sum, dz = plus + minus, plus - minus
        store_rows(a_ref, at, a[:ny], a[ny:])
        a_up, a_down = load_rows(a_ref, at, 1, ny), load_rows(a_ref, at, -1, ny)
        dy = a_up - a_down
        t_ref[at] = (a + a) + ((a_up + a_down) + z_sum)
        dy_ref[at] = dy
        dz_ref[at] = dz
        if -2 < x < nx + 1:
            store_rows(zs_ref, at, z_sum[:ny], z_sum[ny:])
            gy_ref[k, x + 1] = (dy + dy) + (load_rows(zs_ref, at, 1, ny) - load_rows(zs_ref, at, -1, ny))
            store_rows(a_ref, at, dz[:ny], dz[ny:])
            gz_ref[k, x + 1] = (dz + dz) + (load_rows(a_ref, at, 1, ny) + load_rows(a_ref, at, -1, ny))

    def speed(k, common, gradient):
        return [common[a] - (COUPLING * TAU[k] * W2) * gradient[a] for a in range(3)]

    def collide(k, x):
        n, other = x + 1, 1 - k
        gradient = (
            t_ref[other, n + 2] - t_ref[other, n],
            gy_ref[other, n] + (dy_ref[other, n + 2] + dy_ref[other, n]),
            gz_ref[other, n] + (dz_ref[other, n + 2] + dz_ref[other, n]),
        )
        common = []
        for a in range(3):
            main = from_below[2 + a] if x < 0 else from_above[2 + a] if x == nx else field[2 + a, x]
            common.append(jnp.concatenate([main, rows(com(a, x))], axis=0))
        own = signed(k, x)

        def population(i):
            if x < 0:
                main = from_below[5 + XP.index(i)]
            elif x == nx:
                main = from_above[5 + XM.index(i)]
            else:
                main = pop[1, i, x]
            if not VEL[i][1]:
                return False, main
            j = next(j for j, both in enumerate(YPAIR) if i in both)
            return True, jnp.concatenate([main, rows(low if x < 0 else high if x == nx else pair(j, x))], axis=0)

        dirs = XP if x < 0 else XM if x == nx else range(19)
        for i, value in posts(k, jnp.abs(own), speed(k, common, gradient), own > 0.0, dirs, population).items():
            if VEL[i][1]:
                store_rows(post_ref, (k, i, n), value[:ny], value[ny:])
            else:
                post_ref[k, i, n, 8 : 8 + ny] = value

    half = nz // 2

    def collide_sheets(k):
        is_low = lane < half
        part = lambda one, f, two, g: jnp.where(is_low, roll(one, -f * wide, 1), roll(two, half - g * wide, 1))
        right, left = (lambda v: roll(v, -1, 1)), (lambda v: roll(v, 1, 1))
        other = 1 - k
        own, a = part(z_lo, k, z_hi, k), jnp.abs(part(z_lo, other, z_hi, other))
        plus = jnp.abs(part(own_lo, other, own_hi, other))
        minus = jnp.abs(part(z_lo, 10 + other, z_hi, 10 + other))
        a_up, a_down = up(a), down(a)
        z_sum, dz, dy = plus + minus, plus - minus, a_up - a_down
        t = (a + a) + (a_up + a_down + z_sum)
        gradient = (
            right(t) - left(t),
            (dy + dy) + (up(z_sum) - down(z_sum) + right(dy) + left(dy)),
            (dz + dz) + (up(dz) + down(dz) + right(dz) + left(dz)),
        )
        common = [part(z_lo, 2 + a, z_hi, 2 + a) for a in range(3)]
        common[2] = jnp.where(is_low, common[2], -common[2])
        population = lambda i: (True, part(z_lo, 5 + ZP.index(i), z_hi, 5 + ZM.index(mirror(i))) if k else None)
        for i, value in posts(k, jnp.abs(own), speed(k, common, gradient), own > 0.0, ZP, population).items():
            edge_ref[k, ZP.index(i)] = roll(value, VEL[i][1], 0)[:ny]

    lane_of = lanes((ny, nz))

    def write(k, x):
        return pltpu.make_async_copy(out.at[k, :, x], out_hbm.at[k, :, x], sems.at[k, x])

    def finish(k, x):
        fluid = solid[x] == 0
        for i in range(19):
            cx, cy, cz = VEL[i]
            source = x - cx
            value = post_ref[k, i, source + 1, 8 - cy : 8 - cy + ny]
            if cz == 1:
                edge = roll(edge_ref[k, ZP.index(i)], -(source + 2), 1)
                value = jnp.where(lane_of == 0, edge, roll(value, 1, 1))
            elif cz == -1:
                edge = roll(edge_ref[k, ZP.index(mirror(i))], nz - 1 - half - (source + 2), 1)
                value = jnp.where(lane_of == nz - 1, edge, roll(value, -1, 1))
            if i:
                value = jnp.where(value < LIMIT, value, post_ref[k, OPP[i], x + 1, 8 : 8 + ny])
            out[k, i, x] = jnp.where(fluid, value, pop[k, i, x])
        write(k, x).start()

    for x in range(-2, 4):
        shift_psi(1, x)
    collide_sheets(0)
    for x in range(-1, 2):
        collide(0, x)
    later = [functools.partial(shift_psi, 0, x) for x in range(-2, nx + 2)]
    later += [functools.partial(collide_sheets, 1)] + [functools.partial(collide, 1, x) for x in range(-1, 2)]
    share = -(-len(later) // nx)
    for x in range(nx):
        if x + 4 < nx + 2:
            shift_psi(1, x + 4)
        if x + 2 < nx + 1:
            collide(0, x + 2)
        finish(0, x)
        for task in later[x * share : (x + 1) * share]:
            task()
    for x in range(nx):
        if x + 2 < nx + 1:
            collide(1, x + 2)
        finish(1, x)
    for k in range(2):
        for x in range(nx):
            write(k, x).wait()


def ring(value, axis, count, step):
    return lax.ppermute(value, axis, [(i, (i + step) % count) for i in range(count)])


def spread(high, low, axis, count):
    return ring(high, axis, count, 1), ring(low, axis, count, -1)


def spread_rows(rows, count):
    return spread(rows, rows, "gy", count) if count > 2 else (ring(rows, "gy", count, 1),)


def call(kernel, out_shape, *args, scratch=(), hbm_in=0, hbm_out=0, flops=200000, limit=16 * 2**20):
    space = lambda n, held: [pl.BlockSpec(memory_space=pltpu.HBM if j < held else pltpu.VMEM) for j in range(n)]
    args = [pltpu.with_memory_space_constraint(v, pltpu.HBM) if j < hbm_in else v for j, v in enumerate(args)]
    return pl.pallas_call(
        kernel,
        out_shape=[jax.ShapeDtypeStruct(*(s if isinstance(s[-1], type) else (s, jnp.float32))) for s in out_shape],
        in_specs=space(len(args), hbm_in),
        out_specs=space(len(out_shape), hbm_out),
        scratch_shapes=list(scratch),
        compiler_params=pltpu.CompilerParams(vmem_limit_bytes=limit),
        cost_estimate=pl.CostEstimate(flops=flops, bytes_accessed=flops, transcendentals=0),
    )(*args)


def body(sizes, pop, solid):
    return step(sizes, pop, solid)


def step(sizes, pop, solid):
    nx, ny, nz = solid.shape
    count = y_index(nx)[-1]
    wide = nx + 4
    face, plane, tall, padded = (HALO, ny, nz), (ny, nz), (ny + 8, nz), (ny + 16, nz)
    gx, gy, gz = sizes["gx"], sizes["gy"], sizes["gz"]
    y_parts = 1 if gy == 2 else 2
    field, face_high, face_low, rim_high, rim_low, pop_v, solid_v = call(
        first_kernel,
        [(5, nx, ny, nz), face, face, plane, plane, pop.shape, (solid.shape, jnp.int32)],
        pop, solid,
        scratch=[pltpu.SemaphoreType.DMA((nx + 1,))],
        hbm_in=2,
    )
    rims = spread(rim_high, rim_low, "gx", gx)
    faces = spread(face_high, face_low, "gx", gx)
    (sheets,) = call(column_kernel, [(2,) + plane], field, pop_v)
    joined, ends = call(functools.partial(join_kernel, nx), [(2,) + plane, (2, 8, nz)], sheets, *rims)
    ends = spread_rows(ends, gy)
    own = call(functools.partial(z_kernel, y_parts), [tall, tall], joined, *ends)
    far = spread(*own, "gz", gz)
    (rows,) = call(functools.partial(y_kernel, nx), [(count, 8, nz)], field, pop_v, *faces)
    from_y = spread_rows(rows, gy)
    vmem = lambda *s: pltpu.VMEM(s, jnp.float32)
    (result,) = call(
        functools.partial(last_kernel, nx, y_parts),
        [pop.shape],
        pop_v, solid_v, field, *own, *faces, *far, *from_y,
        scratch=[vmem(*pop.shape), vmem(2, wide, *padded)]
        + [vmem(2, wide, *tall)] * 3
        + [vmem(2, wide, *padded)]
        + [vmem(2, nx + 2, *tall)] * 2
        + [vmem(2, 19, nx + 2, *padded), vmem(2, 5, ny, nz), pltpu.SemaphoreType.DMA((2, nx))],
        hbm_out=1,
    )
    return result


def solution(mesh):
    sizes = dict(mesh.shape)
    spec = P(None, None, "gx", "gy", "gz")
    return jax.shard_map(
        functools.partial(body, sizes),
        mesh=mesh,
        in_specs=(spec, P("gx", "gy", "gz")),
        out_specs=spec,
        check_vma=False,
    )
```
